512 devices in a mesh: dom: 8 (over z_lo), col: 8 (over y, core), rep: 8 (over z_hi, x).
Axes of the slice: x: 4, y: 4, z: 16 (z_hi: 2, z_lo: 8; z = z_hi * 8 + z_lo), core: 2. Of those that a mesh axis runs over, the one named last changes fastest.
Arguments:
- features: bfloat16 [8, 8192, 100], P('rep', 'dom'), may hold values from -6 to 6
- w_in: bfloat16 [100, 256], P(None, 'col'), may hold values from -0.625 to 0.625
- w_hidden: bfloat16 [256, 256], P('col'), may hold values from -0.375 to 0.375
- blocks: bfloat16 [8, 8, 8, 512, 512], P('rep', 'dom'), may hold values from -0.125 to 0.125
- block_list: int32 [8, 8, 8, 3], P('rep', 'dom'), may hold values from 0 to 7, as said below
- block_count: int32 [8, 8], P('rep', 'dom'), may hold values from 1 to 8, as said below
- cotangent: bfloat16 [8, 8192, 256], P('rep', 'dom', 'col'), may hold values from -6 to 6
Outputs:
- out_hidden: bfloat16 [8, 8192, 256], P('rep', 'dom', 'col')
- grad_hidden: float32 [256, 256], P('col', ('dom', 'rep'))
The draws below stay inside these ranges and needn't reach their ends.
Inputs may be any that keep to these rules, and one draw needn't show every extreme that they name: `block_list`: each slot holds a row cluster below 2, a partner partition below 8 and a partner cluster below 2; the same cluster pair may stand in several slots, and then their blocks add. `block_count`: in every batch some partition uses all 8 slots.
All inputs are finite; a program needn't handle non-finite values.
Results may differ from the reference program's by a relative error of at most 0.0065.
Values may be sent and summed in bfloat16 or wider, within the bound.
A program may use at most 64 MiB of HBM per device.

```python
import jax
import jax.numpy as jnp
from jax import lax

FEATS = 100
HID = 256
CLUS = 512
SLOTS = 8
CL_DEV = 2
NODES = 8192
N_DOM = 8
N_REP = 8


def draw_block_list(key, part):
    first, second, third = jax.random.split(jax.random.fold_in(key, 11), 3)
    shape = (N_REP, N_DOM, SLOTS)
    row_cluster = jax.random.randint(first, shape, 0, CL_DEV)
    partner = jax.random.randint(second, shape, 0, N_DOM)
    partner_cluster = jax.random.randint(third, shape, 0, CL_DEV)
    return jnp.stack([row_cluster, partner, partner_cluster], axis=-1).astype(jnp.int32)


def draw_block_count(key, part):
    first, second = jax.random.split(jax.random.fold_in(key, 23))
    counts = jax.random.randint(first, (N_REP, N_DOM), 1, SLOTS + 1)
    busiest = jax.random.randint(second, (N_REP,), 0, N_DOM)
    hit = jnp.arange(N_DOM)[None, :] == busiest[:, None]
    return jnp.where(hit, SLOTS, counts).astype(jnp.int32)


def shard_levels(stream_key, shape, pieces, smallest, top_value):
    level, own = 1.0, jax.random.fold_in(stream_key, 6)
    for dim, shards_of in pieces:
        steps = jnp.exp(jax.random.uniform(jax.random.fold_in(own, dim), (shards_of,), jnp.float32, smallest / len(pieces), top_value / len(pieces)))
        level = level * jnp.repeat(steps, shape[dim] // shards_of).reshape([-1 if axis == dim else 1 for axis in range(len(shape))])
    return level


def normal_values(key, dims, deviation, reach, cuts=(), kind=jnp.bfloat16):
    values = jax.random.normal(key, dims, jnp.float32) * deviation
    if len(cuts) > 0:
        values = shard_levels(key, dims, cuts, -0.22, 0.18) * values
    return jnp.clip(values, min=-reach, max=reach).astype(kind)


def setup_inputs(seed: int = 0) -> dict:
    streams_of = jax.random.split(jax.random.key(seed), 8)
    features = normal_values(streams_of[0], (N_REP, NODES, FEATS), 1.0, 6.0, ((0, 8), (1, 8)))
    w_in = normal_values(streams_of[1], (FEATS, HID), FEATS ** -0.5, 0.625, ((1, 8),))
    w_hidden = normal_values(streams_of[2], (HID, HID), HID ** -0.5, 0.375, ((0, 8),))
    blocks = normal_values(streams_of[3], (N_REP, N_DOM, SLOTS, CLUS, CLUS), (4 * CLUS) ** -0.5, 0.125, ((0, 8), (1, 8)))
    block_list = draw_block_list(jax.random.fold_in(streams_of[7], 71), 0)
    block_count = draw_block_count(jax.random.fold_in(streams_of[7], 71), 0)
    cotangent = normal_values(streams_of[6], (N_REP, NODES, HID), 1.0, 6.0, ((0, 8), (1, 8), (2, 8)))
    return {"features": features, "w_in": w_in, "w_hidden": w_hidden, "blocks": blocks, "block_list": block_list, "block_count": block_count, "cotangent": cotangent}


def slot_tables(block_list, block_count):
    rows_dev = CL_DEV * CLUS
    lists = block_list.reshape(N_DOM * SLOTS, 3).astype(jnp.int32)
    owner = jnp.repeat(jnp.arange(N_DOM, dtype=jnp.int32), SLOTS)
    live = (jnp.arange(SLOTS, dtype=jnp.int32)[None, :] < block_count[:, None]).reshape(-1)
    target = (owner * rows_dev + lists[:, 0] * CLUS).astype(jnp.int32)
    source = (lists[:, 1] * rows_dev + lists[:, 2] * CLUS).astype(jnp.int32)
    return target, source, live


def propagate(flat_blocks, target, source, live, values, adjoint):
    width = values.shape[1]
    total = jnp.zeros((values.shape[0], width), jnp.float32)

    def one(acc, item):
        block, into, frm, used = item
        if adjoint:
            frm, into = into, frm
            part = lax.dynamic_slice_in_dim(values, frm, CLUS, 0)
            term = lax.dot_general(block, part, (((0,), (0,)), ((), ())), preferred_element_type=jnp.float32)
        else:
            part = lax.dynamic_slice_in_dim(values, frm, CLUS, 0)
            term = jnp.dot(block, part, preferred_element_type=jnp.float32)
        term = jnp.where(used, term, jnp.zeros_like(term))
        current = lax.dynamic_slice_in_dim(acc, into, CLUS, 0)
        return lax.dynamic_update_slice_in_dim(acc, current + term, into, 0), None

    total, _ = lax.scan(one, total, (flat_blocks, target, source, live))
    return total


def one_batch(item, w_in, w_hidden):
    feats, blocks, block_list, block_count, cotangent = item
    flat_blocks = blocks.reshape(N_DOM * SLOTS, CLUS, CLUS)
    target, source, live = slot_tables(block_list, block_count)
    z1 = jnp.dot(feats, w_in, preferred_element_type=jnp.float32).astype(jnp.bfloat16)
    p1 = propagate(flat_blocks, target, source, live, z1, False)
    h1 = jax.nn.gelu(p1, approximate=True).astype(jnp.bfloat16)
    z2 = jnp.dot(h1, w_hidden, preferred_element_type=jnp.float32).astype(jnp.bfloat16)
    p2 = propagate(flat_blocks, target, source, live, z2, False).astype(jnp.bfloat16)
    dz2 = propagate(flat_blocks, target, source, live, cotangent, True).astype(jnp.bfloat16)
    grad = lax.dot_general(h1, dz2, (((0,), (0,)), ((), ())), preferred_element_type=jnp.float32)
    return p2, grad


def reference(features, w_in, w_hidden, blocks, block_list, block_count, cotangent):
    outs, grads = lax.map(lambda item: one_batch(item, w_in, w_hidden), (features, blocks, block_list, block_count, cotangent))
    return outs, jnp.sum(grads, axis=0)
```

```python
import functools

import jax
import jax.numpy as jnp
from jax import lax
from jax.experimental import pallas as pl
from jax.experimental.pallas import tpu as pltpu
from jax.sharding import PartitionSpec as P

F32 = jnp.float32
BF16 = jnp.bfloat16
MESH = pl.DeviceIdType.MESH
NT = (((1,), (1,)), ((), ()))
CHUNKS = 4


def gelu(v):
    return 0.5 * v * (1.0 + jnp.tanh(0.7978845608028654 * (v + 0.044715 * (v * v * v))))


def kernel(
    dims,
    list_ref, count_ref, feat_hbm, win_hbm, wh_hbm, blocks_hbm, ct_hbm,
    out_ref, grad_ref,
    feat, win, blocks, z1, z2, ctb, ctp, wb, wct, gb, pb, rb, zb, zr,
    local_sem, line_send, line_recv, in_send, in_recv, ring_send, ring_recv,
    x_send, x_recv, z_send, z_recv,
):
    n_dom, n_col, n_x = dims
    n_y, n_z = n_col // 2, 2 * n_dom
    dom, col, rep = lax.axis_index("dom"), lax.axis_index("col"), lax.axis_index("rep")
    y, core = col // 2, col % 2
    z_hi, x = rep // n_x, rep % n_x
    z = z_hi * n_dom + dom

    def on_z(step):
        there = lax.rem(z + step, n_z)
        return {"dom": lax.rem(there, n_dom), "rep": (there // n_dom) * n_x + x}

    def on_x(step):
        return {"rep": z_hi * n_x + lax.rem(x + step, n_x)}

    def on_col(step):
        return {"col": lax.rem(col + step, n_col)}

    def on_y(step):
        return {"col": 2 * lax.rem(y + step, n_y) + core}

    sibling = {"col": 2 * y + 1 - core}

    def send(src, dst, send_sem, recv_sem, device):
        return pltpu.make_async_remote_copy(
            src_ref=src, dst_ref=dst, send_sem=send_sem, recv_sem=recv_sem,
            device_id=device, device_id_type=MESH,
        )

    barrier = pltpu.get_barrier_semaphore()
    for steps, place in ((n_z, on_z), (n_x, on_x), (n_col, on_col)):
        def greet(step, carry, place=place):
            pl.semaphore_signal(barrier, inc=1, device_id=place(step), device_id_type=MESH)
            return carry

        lax.fori_loop(1, steps, greet, 0)

    loads = [
        pltpu.make_async_copy(feat_hbm, feat, local_sem.at[0]),
        pltpu.make_async_copy(win_hbm, win, local_sem.at[1]),
        pltpu.make_async_copy(ct_hbm, ctb.at[col], local_sem.at[2]),
        pltpu.make_async_copy(wh_hbm, wb.at[col], local_sem.at[3]),
        pltpu.make_async_copy(blocks_hbm, blocks, local_sem.at[4]),
    ]
    for load in loads:
        load.start()

    def line_copy(e, buf, src, chunk, way):
        part = buf.at[2 * src + chunk // 2, chunk % 2]
        there = dom + 1 if way == 0 else dom - 1
        return send(
            part, part, line_send.at[e, way, src, chunk], line_recv.at[e, src, chunk],
            {"dom": there},
        )

    def line_start(e, buf):
        for chunk in range(CHUNKS):
            @pl.when(dom < n_dom - 1)
            def _():
                line_copy(e, buf, dom, chunk, 0).start()

            @pl.when(dom > 0)
            def _():
                line_copy(e, buf, dom, chunk, 1).start()

    def line_pass(e, buf):
        def step(s, carry):
            for chunk in range(CHUNKS):
                @pl.when(dom - s >= 0)
                def _():
                    line_copy(e, buf, dom - s, chunk, 0).wait_recv()

                    @pl.when(dom < n_dom - 1)
                    def _():
                        line_copy(e, buf, dom - s, chunk, 0).start()

                @pl.when(dom + s < n_dom)
                def _():
                    line_copy(e, buf, dom + s, chunk, 1).wait_recv()

                    @pl.when(dom > 0)
                    def _():
                        line_copy(e, buf, dom + s, chunk, 1).start()
            return carry

        lax.fori_loop(1, n_dom, step, 0)

    def line_drain(e, buf):
        def step(src, carry):
            for chunk in range(CHUNKS):
                @pl.when((src <= dom) & (dom < n_dom - 1))
                def _():
                    line_copy(e, buf, src, chunk, 0).wait_send()

                @pl.when((src >= dom) & (dom > 0))
                def _():
                    line_copy(e, buf, src, chunk, 1).wait_send()
            return carry

        lax.fori_loop(0, n_dom, step, 0)

    def gather_copy(a, buf, step):
        return send(buf.at[col], buf.at[col], in_send.at[a, step], in_recv.at[a, col], on_col(step))

    def gather_arrival(a, buf, step):
        src = lax.rem(col + step, n_col)
        return send(buf.at[src], buf.at[src], in_send.at[a, step], in_recv.at[a, src], on_col(step))

    def spread(buf):
        total = jnp.zeros((64, 512), F32)
        for slot in range(8):
            used = slot < count_ref[0, 0]
            row = list_ref[0, slot]
            part = buf[2 * list_ref[1, slot] + list_ref[2, slot]].reshape(32, 512).astype(F32)
            first = jnp.where(used & (row == 0), 1.0, 0.0)
            second = jnp.where(used & (row == 1), 1.0, 0.0)
            both = jnp.concatenate([part * first, part * second], axis=0).astype(BF16)
            total = total + lax.dot_general(both, blocks[slot], NT, preferred_element_type=F32)
        return total

    loads[0].wait()
    loads[1].wait()
    own = jnp.dot(win[...], feat[...], preferred_element_type=F32).astype(BF16)
    for j in range(2):
        for h in range(2):
            z1[2 * dom + j, h] = own[16 * h : 16 * h + 16, 512 * j : 512 * j + 512]

    pl.semaphore_wait(barrier, (n_z - 1) + (n_x - 1) + (n_col - 1))
    line_start(0, z1)

    loads[2].wait()
    loads[3].wait()
    for a, buf in ((0, wb), (1, ctb)):
        def start(step, carry, a=a, buf=buf):
            gather_copy(a, buf, step).start()
            return carry

        lax.fori_loop(1, n_col, start, 0)

    line_pass(0, z1)
    loads[4].wait()
    h1 = gelu(spread(z1)).astype(BF16)
    for j in range(2):
        for h in range(2):
            z2[2 * dom + j, h] = h1[32 * j + 16 * h : 32 * j + 16 * h + 16]
    line_start(1, z2)

    for a, buf in ((0, wb), (1, ctb)):
        def arrive(step, carry, a=a, buf=buf):
            gather_arrival(a, buf, step).wait_recv()
            return carry

        lax.fori_loop(1, n_col, arrive, 0)
    units = lax.broadcasted_iota(jnp.int32, (32, 256), 0) + 32 * col
    pick = (lax.broadcasted_iota(jnp.int32, (32, 256), 1) == units).astype(F32).astype(BF16)
    wct[...] = lax.dot_general(
        pick, wb[...].reshape(256, 256), NT, preferred_element_type=F32
    ).astype(BF16)
    place = lax.broadcasted_iota(jnp.int32, (256, 256), 0)
    wanted = 32 * (place & 7) + 16 * ((place >> 3) & 1) + 4 * ((place >> 4) & 3) + (place >> 6)
    order = (lax.broadcasted_iota(jnp.int32, (256, 256), 1) == wanted).astype(F32).astype(BF16)
    ctp[...] = jnp.dot(
        order, ctb[...].reshape(256, 1024), preferred_element_type=F32
    ).astype(BF16)

    line_pass(1, z2)
    g = spread(z2).astype(BF16)
    for j in range(2):
        for h in range(2):
            gb[col, h, :, 512 * j : 512 * j + 512] = g[32 * j + 16 * h : 32 * j + 16 * h + 16]

    def ring_copy(index, src, h, device):
        part = gb.at[src] if h is None else gb.at[src, h]
        return send(part, part, ring_send.at[index], ring_recv.at[index], device)

    before = 2 * lax.rem(y + n_y - 1, n_y) + core
    after = 2 * lax.rem(y + 1, n_y) + core
    across = 2 * lax.rem(y + 2, n_y) + core
    up, down = on_y(1), on_y(n_y - 1)
    other = 1 - 2 * core
    first = [
        ring_copy(0, col, 0, up), ring_copy(1, col, 1, down),
        ring_copy(2, col, 1, up), ring_copy(3, col, 0, down),
        ring_copy(4, col, None, sibling),
    ]
    for copy in first:
        copy.start()

    ga = gb[col].reshape(32, 1024)
    part = lax.dot_general(ctp[...], ga, NT, preferred_element_type=F32)
    packed = jnp.concatenate([part[64 * q : 64 * q + 64] for q in range(4)], axis=1)
    for t in range(n_x):
        pb[t] = packed[16 * t : 16 * t + 16]

    def x_copy(step):
        return send(
            pb.at[lax.rem(x + step, n_x)], rb.at[step], x_send.at[step], x_recv.at[step], on_x(step)
        )

    for step in range(1, n_x):
        x_copy(step).start()

    ring_copy(0, before, 0, up).wait_recv()
    second = [ring_copy(5, before, 0, up)]
    second[0].start()
    ring_copy(1, after, 1, down).wait_recv()
    second.append(ring_copy(6, after, 1, down))
    second[1].start()
    ring_copy(2, before, 1, up).wait_recv()
    second.append(ring_copy(7, before, None, sibling))
    second[2].start()
    ring_copy(3, after, 0, down).wait_recv()
    second.append(ring_copy(8, after, None, sibling))
    second[3].start()

    sums = pb[x]
    for step in range(1, n_x):
        x_copy(step).wait_recv()
        sums = sums + rb[step]
    for t in range(n_z):
        zb[t] = sums[t : t + 1]

    def z_copy(step):
        return send(
            zb.at[lax.rem(z + step, n_z)], zr.at[step], z_send.at[step], z_recv.at[step], on_z(step)
        )

    def z_start(step, carry):
        z_copy(step).start()
        return carry

    lax.fori_loop(1, n_z, z_start, 0)

    ring_copy(5, across, 0, up).wait_recv()
    third = [ring_copy(9, across, 0, sibling)]
    third[0].start()
    ring_copy(6, across, 1, down).wait_recv()
    third.append(ring_copy(10, across, 1, sibling))
    third[1].start()
    ring_copy(4, col + other, None, sibling).wait_recv()
    ring_copy(7, before + other, None, sibling).wait_recv()
    ring_copy(8, after + other, None, sibling).wait_recv()
    ring_copy(9, across + other, 0, sibling).wait_recv()
    ring_copy(10, across + other, 1, sibling).wait_recv()
    out_ref[...] = jnp.dot(
        wct[...], gb[...].reshape(256, 1024), preferred_element_type=F32
    ).astype(BF16)

    def z_add(step, total):
        z_copy(step).wait_recv()
        return total + zr[step]

    total = lax.fori_loop(1, n_z, z_add, zb[z])
    for q in range(4):
        grad_ref[q : q + 1, :] = total[:, 32 * q : 32 * q + 32]

    for copy in first + second + third:
        copy.wait_send()
    for step in range(1, n_x):
        x_copy(step).wait_send()

    def z_done(step, carry):
        z_copy(step).wait_send()
        return carry

    lax.fori_loop(1, n_z, z_done, 0)
    for a, buf in ((0, wb), (1, ctb)):
        def done(step, carry, a=a, buf=buf):
            gather_copy(a, buf, step).wait_send()
            return carry

        lax.fori_loop(1, n_col, done, 0)
    line_drain(0, z1)
    line_drain(1, z2)


def solution(mesh):
    n_dom, n_col = mesh.shape["dom"], mesh.shape["col"]
    n_x = mesh.shape["rep"] // 2
    dims = (n_dom, n_col, n_x)
    n_z = 2 * n_dom

    def body(features, w_in, w_hidden, blocks, block_list, block_count, cotangent):
        hbm = pl.BlockSpec(memory_space=pltpu.HBM)
        smem = pl.BlockSpec(memory_space=pltpu.SMEM)
        vmem = pl.BlockSpec(memory_space=pltpu.VMEM)
        dma = pltpu.SemaphoreType.DMA
        out, grad = pl.pallas_call(
            functools.partial(kernel, dims),
            out_shape=(
                jax.ShapeDtypeStruct((32, 1024), BF16),
                jax.ShapeDtypeStruct((4, 32), F32),
            ),
            in_specs=[smem, smem, hbm, hbm, hbm, hbm, hbm],
            out_specs=(vmem, vmem),
            scratch_shapes=[
                pltpu.VMEM((100, 1024), BF16),
                pltpu.VMEM((32, 100), BF16),
                pltpu.VMEM((8, 512, 512), BF16),
                pltpu.VMEM((2 * n_dom, 2, 16, 512), BF16),
                pltpu.VMEM((2 * n_dom, 2, 16, 512), BF16),
                pltpu.VMEM((n_col, 32, 1024), BF16),
                pltpu.VMEM((256, 1024), BF16),
                pltpu.VMEM((n_col, 32, 256), BF16),
                pltpu.VMEM((32, 256), BF16),
                pltpu.VMEM((n_col, 2, 16, 1024), BF16),
                pltpu.VMEM((n_x, 16, 128), F32),
                pltpu.VMEM((n_x, 16, 128), F32),
                pltpu.VMEM((n_z, 1, 128), F32),
                pltpu.VMEM((n_z, 1, 128), F32),
                dma((5,)),
                dma((2, 2, n_dom, CHUNKS)),
                dma((2, n_dom, CHUNKS)),
                dma((2, n_col)),
                dma((2, n_col)),
                dma((11,)),
                dma((11,)),
                dma((n_x,)),
                dma((n_x,)),
                dma((n_z,)),
                dma((n_z,)),
            ],
            compiler_params=pltpu.CompilerParams(collective_id=0, has_side_effects=True),
        )(
            block_list[0, 0].T,
            block_count,
            features[0].T,
            w_in.T,
            w_hidden,
            blocks[0, 0],
            cotangent[0].T,
        )
        return out.T[None], grad.T

    return jax.shard_map(
        body,
        mesh=mesh,
        in_specs=(
            P("rep", "dom", None),
            P(None, "col"),
            P("col", None),
            P("rep", "dom", None, None, None),
            P("rep", "dom", None, None),
            P("rep", "dom"),
            P("rep", "dom", "col"),
        ),
        out_specs=(P("rep", "dom", "col"), P("col", ("dom", "rep"))),
        check_vma=False,
    )
```

```python
import functools

import jax
import jax.numpy as jnp
from jax import lax
from jax.experimental import pallas as pl
from jax.experimental.pallas import tpu as pltpu
from jax.sharding import PartitionSpec as P

F32 = jnp.float32
BF16 = jnp.bfloat16
MESH = pl.DeviceIdType.MESH
NT = (((1,), (1,)), ((), ()))
CHUNKS = 2
PROGRAMS = {
    0: (('s', 0, 0, 2), ('s', 0, 0, 1), ('s', 0, 1, 2), ('s', 0, 1, 1), ('w', 1, 0, -1), ('w', 1, 1, -1), ('w', 2, 0, -1), ('w', 2, 1, -1), ('w', 3, 0, -1), ('w', 4, 0, -1), ('w', 3, 1, -1), ('w', 4, 1, -1), ('w', 5, 0, -1), ('w', 6, 0, -1), ('w', 5, 1, -1), ('w', 6, 1, -1), ('w', 7, 0, -1), ('w', 7, 1, -1)),
    1: (('s', 1, 0, 3), ('s', 1, 0, 2), ('s', 1, 0, 0), ('s', 1, 1, 3), ('s', 1, 1, 2), ('s', 1, 1, 0), ('w', 0, 0, -1), ('w', 2, 0, -1), ('w', 0, 1, -1), ('w', 2, 1, -1), ('w', 3, 0, -1), ('s', 3, 0, 0), ('w', 3, 1, -1), ('s', 3, 1, 0), ('w', 4, 0, -1), ('w', 5, 0, -1), ('s', 5, 0, 0), ('w', 4, 1, -1), ('w', 5, 1, -1), ('s', 5, 1, 0), ('w', 6, 0, -1), ('w', 7, 0, -1), ('s', 7, 0, 0), ('w', 6, 1, -1), ('w', 7, 1, -1), ('s', 7, 1, 0)),
    2: (('s', 2, 0, 4), ('s', 2, 0, 0), ('s', 2, 0, 3), ('s', 2, 0, 1), ('s', 2, 1, 4), ('s', 2, 1, 0), ('s', 2, 1, 3), ('s', 2, 1, 1), ('w', 0, 0, -1), ('s', 0, 0, 4), ('s', 0, 0, 3), ('w', 3, 0, -1), ('w', 0, 1, -1), ('s', 0, 1, 4), ('s', 0, 1, 3), ('w', 3, 1, -1), ('w', 1, 0, -1), ('w', 4, 0, -1), ('s', 4, 0, 0), ('s', 4, 0, 1), ('w', 4, 1, -1), ('s', 4, 1, 0), ('s', 4, 1, 1), ('w', 1, 1, -1), ('w', 5, 0, -1), ('w', 6, 0, -1), ('s', 6, 0, 0), ('s', 6, 0, 1), ('w', 5, 1, -1), ('w', 6, 1, -1), ('s', 6, 1, 0), ('s', 6, 1, 1), ('w', 7, 0, -1), ('w', 7, 1, -1)),
    3: (('s', 3, 0, 5), ('s', 3, 0, 1), ('s', 3, 0, 4), ('s', 3, 0, 2), ('s', 3, 1, 5), ('s', 3, 1, 1), ('s', 3, 1, 4), ('s', 3, 1, 2), ('w', 4, 0, -1), ('w', 4, 1, -1), ('w', 1, 0, -1), ('s', 1, 0, 5), ('s', 1, 0, 4), ('w', 5, 0, -1), ('s', 5, 0, 1), ('s', 5, 0, 2), ('w', 1, 1, -1), ('s', 1, 1, 5), ('s', 1, 1, 4), ('w', 5, 1, -1), ('s', 5, 1, 1), ('s', 5, 1, 2), ('w', 2, 0, -1), ('w', 2, 1, -1), ('w', 6, 0, -1), ('w', 0, 0, -1), ('w', 7, 0, -1), ('s', 7, 0, 1), ('s', 7, 0, 2), ('w', 6, 1, -1), ('w', 0, 1, -1), ('w', 7, 1, -1), ('s', 7, 1, 1), ('s', 7, 1, 2)),
    4: (('s', 4, 0, 6), ('s', 4, 0, 2), ('s', 4, 0, 5), ('s', 4, 0, 3), ('s', 4, 1, 6), ('s', 4, 1, 2), ('s', 4, 1, 5), ('s', 4, 1, 3), ('w', 5, 0, -1), ('w', 5, 1, -1), ('w', 6, 0, -1), ('s', 6, 0, 2), ('s', 6, 0, 3), ('w', 6, 1, -1), ('s', 6, 1, 2), ('s', 6, 1, 3), ('w', 2, 0, -1), ('s', 2, 0, 6), ('s', 2, 0, 5), ('w', 2, 1, -1), ('s', 2, 1, 6), ('s', 2, 1, 5), ('w', 7, 0, -1), ('w', 3, 0, -1), ('w', 7, 1, -1), ('w', 3, 1, -1), ('w', 0, 0, -1), ('s', 0, 0, 6), ('s', 0, 0, 5), ('w', 0, 1, -1), ('s', 0, 1, 6), ('s', 0, 1, 5), ('w', 1, 0, -1), ('w', 1, 1, -1)),
    5: (('s', 5, 0, 3), ('s', 5, 0, 7), ('s', 5, 0, 6), ('s', 5, 0, 4), ('s', 5, 1, 3), ('s', 5, 1, 7), ('s', 5, 1, 6), ('s', 5, 1, 4), ('w', 6, 0, -1), ('w', 6, 1, -1), ('w', 7, 0, -1), ('s', 7, 0, 3), ('s', 7, 0, 4), ('w', 7, 1, -1), ('s', 7, 1, 3), ('s', 7, 1, 4), ('w', 3, 0, -1), ('s', 3, 0, 7), ('s', 3, 0, 6), ('w', 3, 1, -1), ('s', 3, 1, 7), ('s', 3, 1, 6), ('w', 4, 0, -1), ('w', 4, 1, -1), ('w', 1, 0, -1), ('s', 1, 0, 7), ('s', 1, 0, 6), ('w', 1, 1, -1), ('s', 1, 1, 7), ('s', 1, 1, 6), ('w', 2, 0, -1), ('w', 2, 1, -1), ('w', 0, 0, -1), ('w', 0, 1, -1)),
    6: (('s', 6, 0, 4), ('s', 6, 0, 7), ('s', 6, 0, 5), ('s', 6, 1, 4), ('s', 6, 1, 7), ('s', 6, 1, 5), ('w', 7, 0, -1), ('w', 7, 1, -1), ('w', 4, 0, -1), ('s', 4, 0, 7), ('w', 4, 1, -1), ('s', 4, 1, 7), ('w', 5, 0, -1), ('w', 5, 1, -1), ('w', 2, 0, -1), ('s', 2, 0, 7), ('w', 2, 1, -1), ('s', 2, 1, 7), ('w', 3, 0, -1), ('w', 3, 1, -1), ('w', 0, 0, -1), ('s', 0, 0, 7), ('w', 0, 1, -1), ('s', 0, 1, 7), ('w', 1, 0, -1), ('w', 1, 1, -1)),
    7: (('s', 7, 0, 5), ('s', 7, 0, 6), ('s', 7, 1, 5), ('s', 7, 1, 6), ('w', 5, 0, -1), ('w', 5, 1, -1), ('w', 6, 0, -1), ('w', 6, 1, -1), ('w', 3, 0, -1), ('w', 3, 1, -1), ('w', 4, 0, -1), ('w', 4, 1, -1), ('w', 1, 0, -1), ('w', 1, 1, -1), ('w', 2, 0, -1), ('w', 2, 1, -1), ('w', 0, 0, -1), ('w', 0, 1, -1)),
}
PARTNERS = {0: (1, 2), 1: (0, 2, 3), 2: (0, 1, 3, 4), 3: (1, 2, 4, 5), 4: (2, 3, 5, 6), 5: (3, 4, 6, 7), 6: (4, 5, 7), 7: (5, 6)}


def gelu(v):
    return 0.5 * v * (1.0 + jnp.tanh(0.7978845608028654 * (v + 0.044715 * (v * v * v))))


def kernel(
    dims,
    list_hbm, count_hbm, feat_hbm, win_hbm, wh_hbm, blocks_hbm, ct_hbm,
    out_ref, grad_ref,
    feat, win, blocks, z1, z2, ctb, ctp, wb, wct, gb, pb, rb, zb, zr,
    local_sem, line_send, line_recv, in_send, in_recv, ring_send, ring_recv,
    x_send, x_recv, z_send, z_recv, entered, lists, count,
):
    n_dom, n_col, n_x = dims
    n_y, n_z = n_col // 2, 2 * n_dom
    dom, col, rep = lax.axis_index("dom"), lax.axis_index("col"), lax.axis_index("rep")
    y, core = col // 2, col % 2
    z_hi, x = rep // n_x, rep % n_x
    z = z_hi * n_dom + dom

    def on_z(step):
        there = lax.rem(z + step, n_z)
        return {"dom": lax.rem(there, n_dom), "rep": (there // n_dom) * n_x + x}

    def on_x(step):
        return {"rep": z_hi * n_x + lax.rem(x + step, n_x)}

    def on_col(step):
        return {"col": lax.rem(col + step, n_col)}

    def on_y(step):
        return {"col": 2 * lax.rem(y + step, n_y) + core}

    sibling = {"col": 2 * y + 1 - core}

    def send(src, dst, send_sem, recv_sem, device):
        return pltpu.make_async_remote_copy(
            src_ref=src, dst_ref=dst, send_sem=send_sem, recv_sem=recv_sem,
            device_id=device, device_id_type=MESH,
        )

    barrier = pltpu.get_barrier_semaphore()
    for steps, place in ((n_x, on_x), (n_col, on_col)):
        def greet(step, carry, place=place):
            pl.semaphore_signal(barrier, inc=1, device_id=place(step), device_id_type=MESH)
            return carry

        lax.fori_loop(1, steps, greet, 0)
    for v in range(n_dom):
        @pl.when(dom == v)
        def _(v=v):
            for partner in PARTNERS[v]:
                pl.semaphore_signal(
                    barrier, inc=1, device_id={"dom": partner}, device_id_type=MESH
                )
            if v == 0:
                pl.semaphore_signal(barrier, inc=1, device_id=on_z(n_z - 1), device_id_type=MESH)
            if v == n_dom - 1:
                pl.semaphore_signal(barrier, inc=1, device_id=on_z(1), device_id_type=MESH)

    loads = [
        pltpu.make_async_copy(feat_hbm, feat, local_sem.at[0]),
        pltpu.make_async_copy(win_hbm, win, local_sem.at[1]),
        pltpu.make_async_copy(ct_hbm, ctb.at[col], local_sem.at[2]),
        pltpu.make_async_copy(wh_hbm, wb.at[col], local_sem.at[3]),
        pltpu.make_async_copy(blocks_hbm, blocks, local_sem.at[4]),
        pltpu.make_async_copy(list_hbm, lists, local_sem.at[5]),
        pltpu.make_async_copy(count_hbm, count, local_sem.at[6]),
    ]
    for load in loads:
        load.start()

    def piece(buf, src, chunk):
        if CHUNKS == 1:
            return buf.at[2 * src : 2 * src + 2]
        return buf.at[2 * src + chunk]

    def line_copy(e, buf, src, chunk, dst):
        part = piece(buf, src, chunk)
        return send(
            part, part, line_send.at[e, src, chunk, dst], line_recv.at[e, src, chunk], {"dom": dst}
        )

    def for_each_place(steps):
        for v in range(n_dom):
            @pl.when(dom == v)
            def _(v=v):
                steps(v, PROGRAMS[v])

    def line_start(e, buf):
        def steps(v, program):
            for kind, src, chunk, dst in program:
                if kind == "w":
                    return
                line_copy(e, buf, src, chunk, dst).start()

        for_each_place(steps)

    def line_pass(e, buf):
        def steps(v, program):
            waited = False
            for kind, src, chunk, dst in program:
                waited = waited or kind == "w"
                if kind == "w":
                    line_copy(e, buf, src, chunk, v).wait_recv()
                elif waited:
                    line_copy(e, buf, src, chunk, dst).start()

        for_each_place(steps)

    def line_drain(e, buf):
        def steps(v, program):
            for kind, src, chunk, dst in program:
                if kind == "s":
                    line_copy(e, buf, src, chunk, dst).wait_send()

        for_each_place(steps)

    def gather_copy(a, buf, step):
        return send(buf.at[col], buf.at[col], in_send.at[a, step], in_recv.at[a, col], on_col(step))

    def gather_arrival(a, buf, step):
        src = lax.rem(col + step, n_col)
        return send(buf.at[src], buf.at[src], in_send.at[a, step], in_recv.at[a, src], on_col(step))

    def spread(buf):
        total = jnp.zeros((64, 512), F32)
        for slot in range(8):
            used = slot < count[0, 0]
            row = lists[0, 0, 0, slot]
            part = buf[2 * lists[0, 1, 0, slot] + lists[0, 2, 0, slot]].reshape(32, 512).astype(F32)
            first = jnp.where(used & (row == 0), 1.0, 0.0)
            second = jnp.where(used & (row == 1), 1.0, 0.0)
            both = jnp.concatenate([part * first, part * second], axis=0).astype(BF16)
            total = total + lax.dot_general(both, blocks[slot], NT, preferred_element_type=F32)
        return total

    loads[0].wait()
    loads[1].wait()
    own = jnp.dot(win[...], feat[...], preferred_element_type=F32).astype(BF16)
    for j in range(2):
        for h in range(2):
            z1[2 * dom + j, h] = own[16 * h : 16 * h + 16, 512 * j : 512 * j + 512]

    for v in range(n_dom):
        @pl.when(dom == v)
        def _(v=v):
            ends = 1 if v in (0, n_dom - 1) else 0
            pl.semaphore_wait(barrier, len(PARTNERS[v]) + ends + (n_x - 1) + (n_col - 1))

    line_start(0, z1)

    loads[2].wait()
    loads[3].wait()
    for a, buf in ((0, wb), (1, ctb)):
        def start(step, carry, a=a, buf=buf):
            gather_copy(a, buf, step).start()
            return carry

        lax.fori_loop(1, n_col, start, 0)

    line_pass(0, z1)

    @pl.when(dom == n_dom - 1)
    def _():
        pl.semaphore_signal(entered, inc=1, device_id=on_z(1), device_id_type=MESH)

    for load in loads[4:]:
        load.wait()
    h1 = gelu(spread(z1)).astype(BF16)
    for j in range(2):
        for h in range(2):
            z2[2 * dom + j, h] = h1[32 * j + 16 * h : 32 * j + 16 * h + 16]

    @pl.when(dom == 0)
    def _():
        pl.semaphore_wait(entered, 1)

    line_start(1, z2)

    for a, buf in ((0, wb), (1, ctb)):
        def arrive(step, carry, a=a, buf=buf):
            gather_arrival(a, buf, step).wait_recv()
            return carry

        lax.fori_loop(1, n_col, arrive, 0)
    units = lax.broadcasted_iota(jnp.int32, (32, 256), 0) + 32 * col
    pick = (lax.broadcasted_iota(jnp.int32, (32, 256), 1) == units).astype(F32).astype(BF16)
    wct[...] = lax.dot_general(
        pick, wb[...].reshape(256, 256), NT, preferred_element_type=F32
    ).astype(BF16)
    place = lax.broadcasted_iota(jnp.int32, (256, 256), 0)
    wanted = 32 * (place & 7) + 16 * ((place >> 3) & 1) + 4 * ((place >> 4) & 3) + (place >> 6)
    order = (lax.broadcasted_iota(jnp.int32, (256, 256), 1) == wanted).astype(F32).astype(BF16)
    ctp[...] = jnp.dot(
        order, ctb[...].reshape(256, 1024), preferred_element_type=F32
    ).astype(BF16)

    line_pass(1, z2)
    g = spread(z2).astype(BF16)
    for j in range(2):
        for h in range(2):
            gb[col, h, :, 512 * j : 512 * j + 512] = g[32 * j + 16 * h : 32 * j + 16 * h + 16]

    def ring_copy(index, src, h, device):
        part = gb.at[src] if h is None else gb.at[src, h]
        return send(part, part, ring_send.at[index], ring_recv.at[index], device)

    before = 2 * lax.rem(y + n_y - 1, n_y) + core
    after = 2 * lax.rem(y + 1, n_y) + core
    across = 2 * lax.rem(y + 2, n_y) + core
    up, down = on_y(1), on_y(n_y - 1)
    other = 1 - 2 * core
    first = [
        ring_copy(0, col, 0, up), ring_copy(1, col, 1, down),
        ring_copy(2, col, 1, up), ring_copy(3, col, 0, down),
        ring_copy(4, col, None, sibling),
    ]
    for copy in first:
        copy.start()

    ga = gb[col].reshape(32, 1024)
    part = lax.dot_general(ctp[...], ga, NT, preferred_element_type=F32)
    packed = jnp.concatenate([part[64 * q : 64 * q + 64] for q in range(4)], axis=1)
    for t in range(n_x):
        pb[t] = packed[16 * t : 16 * t + 16]

    def x_copy(step):
        return send(
            pb.at[lax.rem(x + step, n_x)], rb.at[step], x_send.at[step], x_recv.at[step], on_x(step)
        )

    for step in range(1, n_x):
        x_copy(step).start()

    sums = pb[x]
    for step in range(1, n_x):
        x_copy(step).wait_recv()
        sums = sums + rb[step]
    for t in range(n_z):
        zb[t] = sums[t : t + 1]

    def z_copy(step):
        return send(
            zb.at[lax.rem(z + step, n_z)], zr.at[step], z_send.at[step], z_recv.at[step], on_z(step)
        )

    def z_start(step, carry):
        z_copy(step).start()
        return carry

    lax.fori_loop(1, n_z, z_start, 0)

    ring_copy(0, before, 0, up).wait_recv()
    second = [ring_copy(5, before, 0, up)]
    second[0].start()
    ring_copy(1, after, 1, down).wait_recv()
    second.append(ring_copy(6, after, 1, down))
    second[1].start()
    ring_copy(2, before, 1, up).wait_recv()
    second.append(ring_copy(7, before, None, sibling))
    second[2].start()
    ring_copy(3, after, 0, down).wait_recv()
    second.append(ring_copy(8, after, None, sibling))
    second[3].start()

    ring_copy(5, across, 0, up).wait_recv()
    third = [ring_copy(9, across, 0, sibling)]
    third[0].start()
    ring_copy(6, across, 1, down).wait_recv()
    third.append(ring_copy(10, across, 1, sibling))
    third[1].start()
    ring_copy(4, col + other, None, sibling).wait_recv()
    ring_copy(7, before + other, None, sibling).wait_recv()
    ring_copy(8, after + other, None, sibling).wait_recv()
    ring_copy(9, across + other, 0, sibling).wait_recv()
    ring_copy(10, across + other, 1, sibling).wait_recv()
    out_ref[...] = jnp.dot(
        wct[...], gb[...].reshape(256, 1024), preferred_element_type=F32
    ).astype(BF16)

    def z_add(step, total):
        z_copy(step).wait_recv()
        return total + zr[step]

    total = lax.fori_loop(1, n_z, z_add, zb[z])
    for q in range(4):
        grad_ref[q : q + 1, :] = total[:, 32 * q : 32 * q + 32]

    for copy in first + second + third:
        copy.wait_send()
    for step in range(1, n_x):
        x_copy(step).wait_send()

    def z_done(step, carry):
        z_copy(step).wait_send()
        return carry

    lax.fori_loop(1, n_z, z_done, 0)
    for a, buf in ((0, wb), (1, ctb)):
        def done(step, carry, a=a, buf=buf):
            gather_copy(a, buf, step).wait_send()
            return carry

        lax.fori_loop(1, n_col, done, 0)
    line_drain(0, z1)
    line_drain(1, z2)


def solution(mesh):
    n_dom, n_col = mesh.shape["dom"], mesh.shape["col"]
    n_x = mesh.shape["rep"] // 2
    dims = (n_dom, n_col, n_x)
    n_z = 2 * n_dom

    def body(features, w_in, w_hidden, blocks, block_list, block_count, cotangent):
        hbm = pl.BlockSpec(memory_space=pltpu.HBM)
        vmem = pl.BlockSpec(memory_space=pltpu.VMEM)
        dma = pltpu.SemaphoreType.DMA
        out, grad = pl.pallas_call(
            functools.partial(kernel, dims),
            out_shape=(
                jax.ShapeDtypeStruct((32, 1024), BF16),
                jax.ShapeDtypeStruct((4, 32), F32),
            ),
            in_specs=[hbm] * 7,
            out_specs=(vmem, vmem),
            scratch_shapes=[
                pltpu.VMEM((100, 1024), BF16),
                pltpu.VMEM((32, 100), BF16),
                pltpu.VMEM((8, 512, 512), BF16),
                pltpu.VMEM((2 * n_dom, 2, 16, 512), BF16),
                pltpu.VMEM((2 * n_dom, 2, 16, 512), BF16),
                pltpu.VMEM((n_col, 32, 1024), BF16),
                pltpu.VMEM((256, 1024), BF16),
                pltpu.VMEM((n_col, 32, 256), BF16),
                pltpu.VMEM((32, 256), BF16),
                pltpu.VMEM((n_col, 2, 16, 1024), BF16),
                pltpu.VMEM((n_x, 16, 128), F32),
                pltpu.VMEM((n_x, 16, 128), F32),
                pltpu.VMEM((n_z, 1, 128), F32),
                pltpu.VMEM((n_z, 1, 128), F32),
                dma((7,)),
                dma((2, n_dom, CHUNKS, n_dom)),
                dma((2, n_dom, CHUNKS)),
                dma((2, n_col)),
                dma((2, n_col)),
                dma((11,)),
                dma((11,)),
                dma((n_x,)),
                dma((n_x,)),
                dma((n_z,)),
                dma((n_z,)),
                pltpu.SemaphoreType.REGULAR,
                pltpu.SMEM((1, 3, 1, 8), jnp.int32),
                pltpu.SMEM((1, 1), jnp.int32),
            ],
            compiler_params=pltpu.CompilerParams(collective_id=0, has_side_effects=True),
        )(
            jnp.transpose(block_list, (0, 3, 1, 2)),
            block_count,
            features[0].T,
            w_in.T,
            w_hidden,
            blocks[0, 0],
            cotangent[0].T,
        )
        return out.T[None], grad.T

    return jax.shard_map(
        body,
        mesh=mesh,
        in_specs=(
            P("rep", "dom", None),
            P(None, "col"),
            P("col", None),
            P("rep", "dom", None, None, None),
            P("rep", "dom", None, None),
            P("rep", "dom"),
            P("rep", "dom", "col"),
        ),
        out_specs=(P("rep", "dom", "col"), P("col", ("dom", "rep"))),
        check_vma=False,
    )
```

```python
import functools

import jax
import jax.numpy as jnp
from jax import lax
from jax.experimental import pallas as pl
from jax.experimental.pallas import tpu as pltpu
from jax.sharding import PartitionSpec as P

F32 = jnp.float32
BF16 = jnp.bfloat16
MESH = pl.DeviceIdType.MESH
NT = (((1,), (1,)), ((), ()))
CHUNKS = 1
PROGRAMS = {
    0: (('s', 0, 0, 1), ('s', 0, 0, 3), ('w', 3, 0, -1), ('s', 3, 0, 1), ('w', 1, 0, -1), ('s', 3, 0, 2), ('w', 2, 0, -1), ('w', 4, 0, -1), ('w', 5, 0, -1), ('w', 6, 0, -1), ('w', 7, 0, -1)),
    1: (('s', 1, 0, 4), ('s', 1, 0, 2), ('w', 0, 0, -1), ('s', 0, 0, 6), ('s', 1, 0, 6), ('s', 1, 0, 0), ('w', 2, 0, -1), ('s', 2, 0, 0), ('w', 4, 0, -1), ('s', 4, 0, 3), ('s', 4, 0, 2), ('s', 4, 0, 0), ('s', 0, 0, 2), ('w', 3, 0, -1), ('w', 7, 0, -1), ('s', 7, 0, 0), ('w', 6, 0, -1), ('w', 5, 0, -1)),
    2: (('s', 2, 0, 5), ('s', 2, 0, 1), ('w', 1, 0, -1), ('s', 2, 0, 3), ('w', 5, 0, -1), ('s', 5, 0, 0), ('s', 5, 0, 3), ('s', 5, 0, 1), ('w', 6, 0, -1), ('w', 7, 0, -1), ('w', 4, 0, -1), ('w', 0, 0, -1), ('w', 3, 0, -1)),
    3: (('s', 3, 0, 6), ('s', 3, 0, 0), ('w', 0, 0, -1), ('s', 0, 0, 5), ('s', 0, 0, 4), ('w', 6, 0, -1), ('s', 6, 0, 0), ('s', 6, 0, 4), ('s', 6, 0, 2), ('w', 2, 0, -1), ('w', 5, 0, -1), ('w', 1, 0, -1), ('w', 7, 0, -1), ('w', 4, 0, -1)),
    4: (('s', 4, 0, 1), ('s', 4, 0, 7), ('w', 1, 0, -1), ('s', 1, 0, 7), ('s', 1, 0, 3), ('s', 1, 0, 5), ('w', 7, 0, -1), ('s', 7, 0, 2), ('s', 7, 0, 3), ('w', 5, 0, -1), ('w', 2, 0, -1), ('w', 0, 0, -1), ('w', 6, 0, -1), ('w', 3, 0, -1)),
    5: (('s', 5, 0, 2), ('s', 5, 0, 6), ('w', 6, 0, -1), ('s', 5, 0, 4), ('w', 2, 0, -1), ('s', 2, 0, 7), ('s', 2, 0, 4), ('s', 2, 0, 6), ('w', 1, 0, -1), ('w', 0, 0, -1), ('w', 3, 0, -1), ('w', 7, 0, -1), ('w', 4, 0, -1)),
    6: (('s', 6, 0, 3), ('s', 6, 0, 5), ('w', 7, 0, -1), ('s', 7, 0, 1), ('s', 6, 0, 1), ('s', 6, 0, 7), ('w', 5, 0, -1), ('s', 5, 0, 7), ('w', 3, 0, -1), ('s', 3, 0, 4), ('s', 3, 0, 5), ('s', 3, 0, 7), ('s', 7, 0, 5), ('w', 4, 0, -1), ('w', 0, 0, -1), ('s', 0, 0, 7), ('w', 1, 0, -1), ('w', 2, 0, -1)),
    7: (('s', 7, 0, 6), ('s', 7, 0, 4), ('w', 4, 0, -1), ('s', 4, 0, 6), ('w', 6, 0, -1), ('s', 4, 0, 5), ('w', 5, 0, -1), ('w', 3, 0, -1), ('w', 2, 0, -1), ('w', 1, 0, -1), ('w', 0, 0, -1)),
}
PARTNERS = {0: (1, 2, 3), 1: (0, 2, 3, 4, 6), 2: (0, 1, 3, 4, 5), 3: (0, 1, 2, 4, 5, 6), 4: (1, 2, 3, 5, 6, 7), 5: (2, 3, 4, 6, 7), 6: (1, 3, 4, 5, 7), 7: (4, 5, 6)}


def gelu(v):
    return 0.5 * v * (1.0 + jnp.tanh(0.7978845608028654 * (v + 0.044715 * (v * v * v))))


def kernel(
    dims,
    list_hbm, count_hbm, feat_hbm, win_hbm, wh_hbm, blocks_hbm, ct_hbm,
    out_ref, grad_ref,
    feat, win, blocks, turned, z1, z2, ctb, ctp, wb, wct, gb, pb, rb, zb, zr,
    local_sem, line_send, line_recv, in_send, in_recv, ring_send, ring_recv,
    x_send, x_recv, z_send, z_recv, entered, lists, count,
):
    n_dom, n_col, n_x = dims
    n_y, n_z = n_col // 2, 2 * n_dom
    dom, col, rep = lax.axis_index("dom"), lax.axis_index("col"), lax.axis_index("rep")
    y, core = col // 2, col % 2
    z_hi, x = rep // n_x, rep % n_x
    z = z_hi * n_dom + dom

    def on_z(step):
        there = lax.rem(z + step, n_z)
        return {"dom": lax.rem(there, n_dom), "rep": (there // n_dom) * n_x + x}

    def on_x(step):
        return {"rep": z_hi * n_x + lax.rem(x + step, n_x)}

    def on_col(step):
        return {"col": lax.rem(col + step, n_col)}

    def on_y(step):
        return {"col": 2 * lax.rem(y + step, n_y) + core}

    sibling = {"col": 2 * y + 1 - core}

    def send(src, dst, send_sem, recv_sem, device):
        return pltpu.make_async_remote_copy(
            src_ref=src, dst_ref=dst, send_sem=send_sem, recv_sem=recv_sem,
            device_id=device, device_id_type=MESH,
        )

    loads = [
        pltpu.make_async_copy(feat_hbm, feat, local_sem.at[0]),
        pltpu.make_async_copy(win_hbm, win, local_sem.at[1]),
        pltpu.make_async_copy(ct_hbm, ctb.at[col], local_sem.at[2]),
        pltpu.make_async_copy(wh_hbm, wb.at[col], local_sem.at[3]),
        pltpu.make_async_copy(blocks_hbm, blocks, local_sem.at[4]),
        pltpu.make_async_copy(list_hbm, lists, local_sem.at[5]),
        pltpu.make_async_copy(count_hbm, count, local_sem.at[6]),
    ]
    for load in loads:
        load.start()

    barrier = pltpu.get_barrier_semaphore()
    for steps, place in ((n_x, on_x), (n_col, on_col)):
        def greet(step, carry, place=place):
            pl.semaphore_signal(barrier, inc=1, device_id=place(step), device_id_type=MESH)
            return carry

        lax.fori_loop(1, steps, greet, 0)
    for v in range(n_dom):
        @pl.when(dom == v)
        def _(v=v):
            for partner in PARTNERS[v]:
                pl.semaphore_signal(
                    barrier, inc=1, device_id={"dom": partner}, device_id_type=MESH
                )
            if v == 0:
                pl.semaphore_signal(barrier, inc=1, device_id=on_z(n_z - 1), device_id_type=MESH)
            if v == n_dom - 1:
                pl.semaphore_signal(barrier, inc=1, device_id=on_z(1), device_id_type=MESH)

    def piece(buf, src, chunk):
        if CHUNKS == 1:
            return buf.at[2 * src : 2 * src + 2]
        return buf.at[2 * src + chunk]

    def line_copy(e, buf, src, chunk, dst):
        part = piece(buf, src, chunk)
        return send(
            part, part, line_send.at[e, src, chunk, dst], line_recv.at[e, src, chunk], {"dom": dst}
        )

    def for_each_place(steps):
        for v in range(n_dom):
            @pl.when(dom == v)
            def _(v=v):
                steps(v, PROGRAMS[v])

    def line_start(e, buf):
        def steps(v, program):
            for kind, src, chunk, dst in program:
                if kind == "w":
                    return
                line_copy(e, buf, src, chunk, dst).start()

        for_each_place(steps)

    def line_pass(e, buf):
        def steps(v, program):
            waited = False
            for kind, src, chunk, dst in program:
                waited = waited or kind == "w"
                if kind == "w":
                    line_copy(e, buf, src, chunk, v).wait_recv()
                elif waited:
                    line_copy(e, buf, src, chunk, dst).start()

        for_each_place(steps)

    def line_drain(e, buf):
        def steps(v, program):
            for kind, src, chunk, dst in program:
                if kind == "s":
                    line_copy(e, buf, src, chunk, dst).wait_send()

        for_each_place(steps)

    def gather_copy(a, buf, step):
        return send(buf.at[col], buf.at[col], in_send.at[a, step], in_recv.at[a, col], on_col(step))

    def gather_arrival(a, buf, step):
        src = lax.rem(col + step, n_col)
        return send(buf.at[src], buf.at[src], in_send.at[a, step], in_recv.at[a, src], on_col(step))

    def spread(buf):
        total = jnp.zeros((64, 512), F32)
        for slot in range(8):
            used = slot < count[0, 0]
            row = lists[0, 0, 0, slot]
            part = buf[2 * lists[0, 1, 0, slot] + lists[0, 2, 0, slot]].reshape(32, 512).astype(F32)
            first = jnp.where(used & (row == 0), 1.0, 0.0)
            second = jnp.where(used & (row == 1), 1.0, 0.0)
            both = jnp.concatenate([part * first, part * second], axis=0).astype(BF16)
            total = total + jnp.dot(both, turned[slot], preferred_element_type=F32)
        return total

    loads[0].wait()
    loads[1].wait()
    own = jnp.dot(win[...], feat[...], preferred_element_type=F32).astype(BF16)
    for j in range(2):
        for h in range(2):
            z1[2 * dom + j, h] = own[16 * h : 16 * h + 16, 512 * j : 512 * j + 512]

    for v in range(n_dom):
        @pl.when(dom == v)
        def _(v=v):
            ends = 1 if v in (0, n_dom - 1) else 0
            pl.semaphore_wait(barrier, len(PARTNERS[v]) + ends + (n_x - 1) + (n_col - 1))

    line_start(0, z1)

    loads[2].wait()
    loads[3].wait()
    for a, buf in ((0, wb), (1, ctb)):
        def start(step, carry, a=a, buf=buf):
            gather_copy(a, buf, step).start()
            return carry

        lax.fori_loop(1, n_col, start, 0)

    for load in loads[4:]:
        load.wait()

    def turn(slot, carry):
        turned[slot] = blocks[slot].T
        return carry

    lax.fori_loop(0, 8, turn, 0)
    line_pass(0, z1)

    @pl.when(dom == n_dom - 1)
    def _():
        pl.semaphore_signal(entered, inc=1, device_id=on_z(1), device_id_type=MESH)

    h1 = gelu(spread(z1)).astype(BF16)
    for j in range(2):
        for h in range(2):
            z2[2 * dom + j, h] = h1[32 * j + 16 * h : 32 * j + 16 * h + 16]

    @pl.when(dom == 0)
    def _():
        pl.semaphore_wait(entered, 1)

    line_start(1, z2)

    for a, buf in ((0, wb), (1, ctb)):
        def arrive(step, carry, a=a, buf=buf):
            gather_arrival(a, buf, step).wait_recv()
            return carry

        lax.fori_loop(1, n_col, arrive, 0)
    units = lax.broadcasted_iota(jnp.int32, (32, 256), 0) + 32 * col
    pick = (lax.broadcasted_iota(jnp.int32, (32, 256), 1) == units).astype(F32).astype(BF16)
    wct[...] = lax.dot_general(
        pick, wb[...].reshape(256, 256), NT, preferred_element_type=F32
    ).astype(BF16)
    place = lax.broadcasted_iota(jnp.int32, (256, 256), 0)
    wanted = 32 * (place & 7) + 16 * ((place >> 3) & 1) + 4 * ((place >> 4) & 3) + (place >> 6)
    order = (lax.broadcasted_iota(jnp.int32, (256, 256), 1) == wanted).astype(F32).astype(BF16)
    ctp[...] = jnp.dot(
        order, ctb[...].reshape(256, 1024), preferred_element_type=F32
    ).astype(BF16)

    line_pass(1, z2)
    g = spread(z2).astype(BF16)
    for j in range(2):
        for h in range(2):
            gb[col, h, :, 512 * j : 512 * j + 512] = g[32 * j + 16 * h : 32 * j + 16 * h + 16]

    def ring_copy(index, src, h, device):
        part = gb.at[src] if h is None else gb.at[src, h]
        return send(part, part, ring_send.at[index], ring_recv.at[index], device)

    before = 2 * lax.rem(y + n_y - 1, n_y) + core
    after = 2 * lax.rem(y + 1, n_y) + core
    across = 2 * lax.rem(y + 2, n_y) + core
    up, down = on_y(1), on_y(n_y - 1)
    other = 1 - 2 * core
    first = [
        ring_copy(0, col, 0, up), ring_copy(1, col, 1, down),
        ring_copy(2, col, 1, up), ring_copy(3, col, 0, down),
        ring_copy(4, col, None, sibling),
    ]
    for copy in first:
        copy.start()

    ga = jnp.concatenate([g[:32], g[32:]], axis=1)
    part = lax.dot_general(ctp[...], ga, NT, preferred_element_type=F32)
    packed = jnp.concatenate([part[64 * q : 64 * q + 64] for q in range(4)], axis=1)
    for t in range(n_x):
        pb[t] = packed[16 * t : 16 * t + 16]

    def x_copy(step):
        return send(
            pb.at[lax.rem(x + step, n_x)], rb.at[step], x_send.at[step], x_recv.at[step], on_x(step)
        )

    for step in range(1, n_x):
        x_copy(step).start()

    sums = pb[x]
    for step in range(1, n_x):
        x_copy(step).wait_recv()
        sums = sums + rb[step]
    for t in range(n_z):
        zb[t] = sums[t : t + 1]

    def z_copy(step):
        return send(
            zb.at[lax.rem(z + step, n_z)], zr.at[step], z_send.at[step], z_recv.at[step], on_z(step)
        )

    def z_start(step, carry):
        z_copy(step).start()
        return carry

    lax.fori_loop(1, n_z, z_start, 0)

    ring_copy(0, before, 0, up).wait_recv()
    second = [ring_copy(5, before, 0, up)]
    second[0].start()
    ring_copy(1, after, 1, down).wait_recv()
    second.append(ring_copy(6, after, 1, down))
    second[1].start()
    ring_copy(2, before, 1, up).wait_recv()
    second.append(ring_copy(7, before, None, sibling))
    second[2].start()
    ring_copy(3, after, 0, down).wait_recv()
    second.append(ring_copy(8, after, None, sibling))
    second[3].start()

    ring_copy(5, across, 0, up).wait_recv()
    third = [ring_copy(9, across, 0, sibling)]
    third[0].start()
    ring_copy(6, across, 1, down).wait_recv()
    third.append(ring_copy(10, across, 1, sibling))
    third[1].start()
    ring_copy(4, col + other, None, sibling).wait_recv()
    ring_copy(7, before + other, None, sibling).wait_recv()
    ring_copy(8, after + other, None, sibling).wait_recv()
    ring_copy(9, across + other, 0, sibling).wait_recv()
    ring_copy(10, across + other, 1, sibling).wait_recv()
    out_ref[...] = jnp.dot(
        wct[...], gb[...].reshape(256, 1024), preferred_element_type=F32
    ).astype(BF16)

    def z_add(step, total):
        z_copy(step).wait_recv()
        return total + zr[step]

    total = lax.fori_loop(1, n_z, z_add, zb[z])
    for q in range(4):
        grad_ref[q : q + 1, :] = total[:, 32 * q : 32 * q + 32]

    for copy in first + second + third:
        copy.wait_send()
    for step in range(1, n_x):
        x_copy(step).wait_send()

    def z_done(step, carry):
        z_copy(step).wait_send()
        return carry

    lax.fori_loop(1, n_z, z_done, 0)
    for a, buf in ((0, wb), (1, ctb)):
        def done(step, carry, a=a, buf=buf):
            gather_copy(a, buf, step).wait_send()
            return carry

        lax.fori_loop(1, n_col, done, 0)
    line_drain(0, z1)
    line_drain(1, z2)


def hand_over(out_in, grad_in, out_ref, grad_ref):
    out_ref[...] = out_in[...]
    grad_ref[...] = grad_in[...]


def solution(mesh):
    n_dom, n_col = mesh.shape["dom"], mesh.shape["col"]
    n_x = mesh.shape["rep"] // 2
    dims = (n_dom, n_col, n_x)
    n_z = 2 * n_dom

    def body(features, w_in, w_hidden, blocks, block_list, block_count, cotangent):
        hbm = pl.BlockSpec(memory_space=pltpu.HBM)
        vmem = pl.BlockSpec(memory_space=pltpu.VMEM)
        dma = pltpu.SemaphoreType.DMA
        out, grad = pl.pallas_call(
            functools.partial(kernel, dims),
            out_shape=(
                jax.ShapeDtypeStruct((32, 1024), BF16),
                jax.ShapeDtypeStruct((4, 32), F32),
            ),
            in_specs=[hbm] * 7,
            out_specs=(vmem, vmem),
            scratch_shapes=[
                pltpu.VMEM((100, 1024), BF16),
                pltpu.VMEM((32, 100), BF16),
                pltpu.VMEM((8, 512, 512), BF16),
                pltpu.VMEM((8, 512, 512), BF16),
                pltpu.VMEM((2 * n_dom, 2, 16, 512), BF16),
                pltpu.VMEM((2 * n_dom, 2, 16, 512), BF16),
                pltpu.VMEM((n_col, 32, 1024), BF16),
                pltpu.VMEM((256, 1024), BF16),
                pltpu.VMEM((n_col, 32, 256), BF16),
                pltpu.VMEM((32, 256), BF16),
                pltpu.VMEM((n_col, 2, 16, 1024), BF16),
                pltpu.VMEM((n_x, 16, 128), F32),
                pltpu.VMEM((n_x, 16, 128), F32),
                pltpu.VMEM((n_z, 1, 128), F32),
                pltpu.VMEM((n_z, 1, 128), F32),
                dma((7,)),
                dma((2, n_dom, CHUNKS, n_dom)),
                dma((2, n_dom, CHUNKS)),
                dma((2, n_col)),
                dma((2, n_col)),
                dma((11,)),
                dma((11,)),
                dma((n_x,)),
                dma((n_x,)),
                dma((n_z,)),
                dma((n_z,)),
                pltpu.SemaphoreType.REGULAR,
                pltpu.SMEM((1, 3, 1, 8), jnp.int32),
                pltpu.SMEM((1, 1), jnp.int32),
            ],
            compiler_params=pltpu.CompilerParams(collective_id=0, has_side_effects=True),
        )(
            jnp.transpose(block_list, (0, 3, 1, 2)),
            block_count,
            features[0].T,
            w_in.T,
            w_hidden,
            blocks[0, 0],
            cotangent[0].T,
        )
        out, grad = pl.pallas_call(
            hand_over,
            out_shape=(
                jax.ShapeDtypeStruct((32, 1024), BF16),
                jax.ShapeDtypeStruct((4, 32), F32),
            ),
            in_specs=[vmem] * 2,
            out_specs=(vmem, vmem),
            compiler_params=pltpu.CompilerParams(vmem_limit_bytes=1024 * 1024),
        )(out, grad)
        return out.T[None], grad.T

    return jax.shard_map(
        body,
        mesh=mesh,
        in_specs=(
            P("rep", "dom", None),
            P(None, "col"),
            P("col", None),
            P("rep", "dom", None, None, None),
            P("rep", "dom", None, None),
            P("rep", "dom"),
            P("rep", "dom", "col"),
        ),
        out_specs=(P("rep", "dom", "col"), P("col", ("dom", "rep"))),
        check_vma=False,
    )
```

```python
import functools

import jax
import jax.numpy as jnp
from jax import lax
from jax.experimental import pallas as pl
from jax.experimental.pallas import tpu as pltpu
from jax.sharding import PartitionSpec as P

F32 = jnp.float32
BF16 = jnp.bfloat16
MESH = pl.DeviceIdType.MESH
NT = (((1,), (1,)), ((), ()))
CHUNKS = 1
PROGRAMS = {
    0: (('s', 0, 0, 1), ('s', 0, 0, 3), ('w', 3, 0, -1), ('s', 3, 0, 1), ('w', 1, 0, -1), ('s', 3, 0, 2), ('w', 2, 0, -1), ('w', 4, 0, -1), ('w', 5, 0, -1), ('w', 6, 0, -1), ('w', 7, 0, -1)),
    1: (('s', 1, 0, 4), ('s', 1, 0, 2), ('w', 0, 0, -1), ('s', 0, 0, 6), ('s', 1, 0, 6), ('s', 1, 0, 0), ('w', 2, 0, -1), ('s', 2, 0, 0), ('w', 4, 0, -1), ('s', 4, 0, 3), ('s', 4, 0, 2), ('s', 4, 0, 0), ('s', 0, 0, 2), ('w', 3, 0, -1), ('w', 7, 0, -1), ('s', 7, 0, 0), ('w', 6, 0, -1), ('w', 5, 0, -1)),
    2: (('s', 2, 0, 5), ('s', 2, 0, 1), ('w', 1, 0, -1), ('s', 2, 0, 3), ('w', 5, 0, -1), ('s', 5, 0, 0), ('s', 5, 0, 3), ('s', 5, 0, 1), ('w', 6, 0, -1), ('w', 7, 0, -1), ('w', 4, 0, -1), ('w', 0, 0, -1), ('w', 3, 0, -1)),
    3: (('s', 3, 0, 6), ('s', 3, 0, 0), ('w', 0, 0, -1), ('s', 0, 0, 5), ('s', 0, 0, 4), ('w', 6, 0, -1), ('s', 6, 0, 0), ('s', 6, 0, 4), ('s', 6, 0, 2), ('w', 2, 0, -1), ('w', 5, 0, -1), ('w', 1, 0, -1), ('w', 7, 0, -1), ('w', 4, 0, -1)),
    4: (('s', 4, 0, 1), ('s', 4, 0, 7), ('w', 1, 0, -1), ('s', 1, 0, 7), ('s', 1, 0, 3), ('s', 1, 0, 5), ('w', 7, 0, -1), ('s', 7, 0, 2), ('s', 7, 0, 3), ('w', 5, 0, -1), ('w', 2, 0, -1), ('w', 0, 0, -1), ('w', 6, 0, -1), ('w', 3, 0, -1)),
    5: (('s', 5, 0, 2), ('s', 5, 0, 6), ('w', 6, 0, -1), ('s', 5, 0, 4), ('w', 2, 0, -1), ('s', 2, 0, 7), ('s', 2, 0, 4), ('s', 2, 0, 6), ('w', 1, 0, -1), ('w', 0, 0, -1), ('w', 3, 0, -1), ('w', 7, 0, -1), ('w', 4, 0, -1)),
    6: (('s', 6, 0, 3), ('s', 6, 0, 5), ('w', 7, 0, -1), ('s', 7, 0, 1), ('s', 6, 0, 1), ('s', 6, 0, 7), ('w', 5, 0, -1), ('s', 5, 0, 7), ('w', 3, 0, -1), ('s', 3, 0, 4), ('s', 3, 0, 5), ('s', 3, 0, 7), ('s', 7, 0, 5), ('w', 4, 0, -1), ('w', 0, 0, -1), ('s', 0, 0, 7), ('w', 1, 0, -1), ('w', 2, 0, -1)),
    7: (('s', 7, 0, 6), ('s', 7, 0, 4), ('w', 4, 0, -1), ('s', 4, 0, 6), ('w', 6, 0, -1), ('s', 4, 0, 5), ('w', 5, 0, -1), ('w', 3, 0, -1), ('w', 2, 0, -1), ('w', 1, 0, -1), ('w', 0, 0, -1)),
}
PARTNERS = {0: (1, 2, 3), 1: (0, 2, 3, 4, 6), 2: (0, 1, 3, 4, 5), 3: (0, 1, 2, 4, 5, 6), 4: (1, 2, 3, 5, 6, 7), 5: (2, 3, 4, 6, 7), 6: (1, 3, 4, 5, 7), 7: (4, 5, 6)}


def gelu(v):
    return 0.5 * v * (1.0 + jnp.tanh(0.7978845608028654 * (v + 0.044715 * (v * v * v))))


def kernel(
    dims,
    list_hbm, count_hbm, feat_hbm, win_hbm, wh_hbm, blocks_hbm, ct_hbm,
    out_ref, grad_ref,
    feat, win, blocks, turned, z1, z2, ctb, ctp, wb, wct, gb, pb, rb, zb, zr,
    local_sem, line_send, line_recv, in_send, in_recv, ring_send, ring_recv,
    x_send, x_recv, z_send, z_recv, entered, lists, count,
):
    n_dom, n_col, n_x = dims
    n_y, n_z = n_col // 2, 2 * n_dom
    dom, col, rep = lax.axis_index("dom"), lax.axis_index("col"), lax.axis_index("rep")
    y, core = col // 2, col % 2
    z_hi, x = rep // n_x, rep % n_x
    z = z_hi * n_dom + dom

    def on_z(step):
        there = lax.rem(z + step, n_z)
        return {"dom": lax.rem(there, n_dom), "rep": (there // n_dom) * n_x + x}

    def on_x(step):
        return {"rep": z_hi * n_x + lax.rem(x + step, n_x)}

    def on_col(step):
        return {"col": lax.rem(col + step, n_col)}

    def on_y(step):
        return {"col": 2 * lax.rem(y + step, n_y) + core}

    sibling = {"col": 2 * y + 1 - core}

    def send(src, dst, send_sem, recv_sem, device):
        return pltpu.make_async_remote_copy(
            src_ref=src, dst_ref=dst, send_sem=send_sem, recv_sem=recv_sem,
            device_id=device, device_id_type=MESH,
        )

    loads = [
        pltpu.make_async_copy(feat_hbm, feat, local_sem.at[0]),
        pltpu.make_async_copy(win_hbm, win, local_sem.at[1]),
        pltpu.make_async_copy(ct_hbm, ctb.at[col], local_sem.at[2]),
        pltpu.make_async_copy(wh_hbm, wb.at[col], local_sem.at[3]),
        pltpu.make_async_copy(blocks_hbm, blocks, local_sem.at[4]),
        pltpu.make_async_copy(list_hbm, lists, local_sem.at[5]),
        pltpu.make_async_copy(count_hbm, count, local_sem.at[6]),
    ]
    for load in loads:
        load.start()

    barrier = pltpu.get_barrier_semaphore()
    for steps, place in ((n_x, on_x), (n_col, on_col)):
        def greet(step, carry, place=place):
            pl.semaphore_signal(barrier, inc=1, device_id=place(step), device_id_type=MESH)
            return carry

        lax.fori_loop(1, steps, greet, 0)
    for v in range(n_dom):
        @pl.when(dom == v)
        def _(v=v):
            for partner in PARTNERS[v]:
                pl.semaphore_signal(
                    barrier, inc=1, device_id={"dom": partner}, device_id_type=MESH
                )

    @pl.when(dom == 0)
    def _():
        pl.semaphore_signal(barrier, inc=1, device_id=on_z(n_z - 1), device_id_type=MESH)

    @pl.when(dom == n_dom - 1)
    def _():
        pl.semaphore_signal(barrier, inc=1, device_id=on_z(1), device_id_type=MESH)

    def piece(buf, src, chunk):
        if CHUNKS == 1:
            return buf.at[2 * src : 2 * src + 2]
        return buf.at[2 * src + chunk]

    def line_copy(e, buf, src, chunk, dst):
        part = piece(buf, src, chunk)
        return send(
            part, part, line_send.at[e, src, chunk, dst], line_recv.at[e, src, chunk], {"dom": dst}
        )

    def for_each_place(steps):
        for v in range(n_dom):
            @pl.when(dom == v)
            def _(v=v):
                steps(v, PROGRAMS[v])

    def line_start(e, buf):
        def steps(v, program):
            for kind, src, chunk, dst in program:
                if kind == "w":
                    return
                line_copy(e, buf, src, chunk, dst).start()

        for_each_place(steps)

    def line_pass(e, buf):
        def steps(v, program):
            waited = False
            for kind, src, chunk, dst in program:
                waited = waited or kind == "w"
                if kind == "w":
                    line_copy(e, buf, src, chunk, v).wait_recv()
                elif waited:
                    line_copy(e, buf, src, chunk, dst).start()

        for_each_place(steps)

    def line_drain(e, buf):
        def steps(v, program):
            for kind, src, chunk, dst in program:
                if kind == "s":
                    line_copy(e, buf, src, chunk, dst).wait_send()

        for_each_place(steps)

    def gather_copy(a, buf, step):
        return send(buf.at[col], buf.at[col], in_send.at[a, step], in_recv.at[a, col], on_col(step))

    def gather_arrival(a, buf, step):
        src = lax.rem(col + step, n_col)
        return send(buf.at[src], buf.at[src], in_send.at[a, step], in_recv.at[a, src], on_col(step))

    def spread(buf):
        total = jnp.zeros((64, 512), F32)
        for slot in range(8):
            used = slot < count[0, 0]
            row = lists[0, 0, 0, slot]
            part = buf[2 * lists[0, 1, 0, slot] + lists[0, 2, 0, slot]].reshape(32, 512).astype(F32)
            first = jnp.where(used & (row == 0), 1.0, 0.0)
            second = jnp.where(used & (row == 1), 1.0, 0.0)
            both = jnp.concatenate([part * first, part * second], axis=0).astype(BF16)
            total = total + jnp.dot(both, turned[slot], preferred_element_type=F32)
        return total

    loads[0].wait()
    loads[1].wait()
    own = jnp.dot(win[...], feat[...], preferred_element_type=F32).astype(BF16)
    for j in range(2):
        for h in range(2):
            z1[2 * dom + j, h] = own[16 * h : 16 * h + 16, 512 * j : 512 * j + 512]

    for v in range(n_dom):
        @pl.when(dom == v)
        def _(v=v):
            ends = 1 if v in (0, n_dom - 1) else 0
            pl.semaphore_wait(barrier, len(PARTNERS[v]) + ends + (n_x - 1) + (n_col - 1))

    line_start(0, z1)

    loads[2].wait()
    loads[3].wait()
    for a, buf in ((0, wb), (1, ctb)):
        def start(step, carry, a=a, buf=buf):
            gather_copy(a, buf, step).start()
            return carry

        lax.fori_loop(1, n_col, start, 0)

    for load in loads[4:]:
        load.wait()

    def turn(slot, carry):
        turned[slot] = blocks[slot].T
        return carry

    lax.fori_loop(0, 8, turn, 0)
    line_pass(0, z1)

    @pl.when(dom == n_dom - 1)
    def _():
        pl.semaphore_signal(entered, inc=1, device_id=on_z(1), device_id_type=MESH)

    h1 = gelu(spread(z1)).astype(BF16)
    for j in range(2):
        for h in range(2):
            z2[2 * dom + j, h] = h1[32 * j + 16 * h : 32 * j + 16 * h + 16]

    @pl.when(dom == 0)
    def _():
        pl.semaphore_wait(entered, 1)

    line_start(1, z2)

    for a, buf in ((0, wb), (1, ctb)):
        def arrive(step, carry, a=a, buf=buf):
            gather_arrival(a, buf, step).wait_recv()
            return carry

        lax.fori_loop(1, n_col, arrive, 0)
    units = lax.broadcasted_iota(jnp.int32, (32, 256), 0) + 32 * col
    pick = (lax.broadcasted_iota(jnp.int32, (32, 256), 1) == units).astype(F32).astype(BF16)
    wct[...] = lax.dot_general(
        pick, wb[...].reshape(256, 256), NT, preferred_element_type=F32
    ).astype(BF16)
    place = lax.broadcasted_iota(jnp.int32, (256, 256), 0)
    wanted = 32 * (place & 7) + 16 * ((place >> 3) & 1) + 4 * ((place >> 4) & 3) + (place >> 6)
    order = (lax.broadcasted_iota(jnp.int32, (256, 256), 1) == wanted).astype(F32).astype(BF16)
    ctp[...] = jnp.dot(
        order, ctb[...].reshape(256, 1024), preferred_element_type=F32
    ).astype(BF16)

    line_pass(1, z2)
    g = spread(z2).astype(BF16)
    for j in range(2):
        for h in range(2):
            gb[col, h, :, 512 * j : 512 * j + 512] = g[32 * j + 16 * h : 32 * j + 16 * h + 16]

    def ring_copy(index, src, h, device):
        part = gb.at[src] if h is None else gb.at[src, h]
        return send(part, part, ring_send.at[index], ring_recv.at[index], device)

    before = 2 * lax.rem(y + n_y - 1, n_y) + core
    after = 2 * lax.rem(y + 1, n_y) + core
    across = 2 * lax.rem(y + 2, n_y) + core
    up, down = on_y(1), on_y(n_y - 1)
    other = 1 - 2 * core
    first = [
        ring_copy(0, col, 0, up), ring_copy(1, col, 1, down),
        ring_copy(2, col, 1, up), ring_copy(3, col, 0, down),
        ring_copy(4, col, None, sibling),
    ]

    for copy in first:
        copy.start()
    ga = jnp.concatenate([g[:32], g[32:]], axis=1)
    part = lax.dot_general(ctp[...], ga, NT, preferred_element_type=F32)
    packed = jnp.concatenate([part[64 * q : 64 * q + 64] for q in range(4)], axis=1)
    for t in range(n_x):
        pb[t] = packed[16 * t : 16 * t + 16]

    def x_copy(step):
        return send(
            pb.at[lax.rem(x + step, n_x)], rb.at[step], x_send.at[step], x_recv.at[step], on_x(step)
        )

    for step in range(1, n_x):
        x_copy(step).start()

    sums = pb[x]
    for step in range(1, n_x):
        x_copy(step).wait_recv()
        sums = sums + rb[step]
    for t in range(n_z):
        zb[t] = sums[t : t + 1]

    def z_copy(step):
        return send(
            zb.at[lax.rem(z + step, n_z)], zr.at[step], z_send.at[step], z_recv.at[step], on_z(step)
        )

    def z_start(step, carry):
        z_copy(step).start()
        return carry

    lax.fori_loop(1, n_z, z_start, 0)

    ring_copy(0, before, 0, up).wait_recv()
    second = [ring_copy(5, before, 0, up)]
    second[0].start()
    ring_copy(1, after, 1, down).wait_recv()
    second.append(ring_copy(6, after, 1, down))
    second[1].start()
    ring_copy(2, before, 1, up).wait_recv()
    second.append(ring_copy(7, before, None, sibling))
    second[2].start()
    ring_copy(3, after, 0, down).wait_recv()
    second.append(ring_copy(8, after, None, sibling))
    second[3].start()

    ring_copy(5, across, 0, up).wait_recv()
    third = [ring_copy(9, across, 0, sibling)]
    third[0].start()
    ring_copy(6, across, 1, down).wait_recv()
    third.append(ring_copy(10, across, 1, sibling))
    third[1].start()
    ring_copy(4, col + other, None, sibling).wait_recv()
    ring_copy(7, before + other, None, sibling).wait_recv()
    ring_copy(8, after + other, None, sibling).wait_recv()
    ring_copy(9, across + other, 0, sibling).wait_recv()
    ring_copy(10, across + other, 1, sibling).wait_recv()
    out_ref[...] = jnp.dot(
        wct[...], gb[...].reshape(256, 1024), preferred_element_type=F32
    ).astype(BF16)

    for copy in first + second + third:
        copy.wait_send()
    for step in range(1, n_x):
        x_copy(step).wait_send()

    for a, buf in ((0, wb), (1, ctb)):
        def done(step, carry, a=a, buf=buf):
            gather_copy(a, buf, step).wait_send()
            return carry

        lax.fori_loop(1, n_col, done, 0)
    line_drain(0, z1)
    line_drain(1, z2)

    def z_add(step, total):
        z_copy(step).wait_recv()
        return total + zr[step]

    total = lax.fori_loop(1, n_z, z_add, zb[z])
    for q in range(4):
        grad_ref[q : q + 1, :] = total[:, 32 * q : 32 * q + 32]

    def z_done(step, carry):
        z_copy(step).wait_send()
        return carry

    lax.fori_loop(1, n_z, z_done, 0)


def hand_over(out_held, grad_held, out_ref, grad_ref, sems):
    copies = [
        pltpu.make_async_copy(out_held, out_ref, sems.at[0]),
        pltpu.make_async_copy(grad_held, grad_ref, sems.at[1]),
    ]
    for copy in copies:
        copy.start()
    for copy in copies:
        copy.wait()


def solution(mesh):
    n_dom, n_col = mesh.shape["dom"], mesh.shape["col"]
    n_x = mesh.shape["rep"] // 2
    dims = (n_dom, n_col, n_x)
    n_z = 2 * n_dom

    def body(features, w_in, w_hidden, blocks, block_list, block_count, cotangent):
        hbm = pl.BlockSpec(memory_space=pltpu.HBM)
        vmem = pl.BlockSpec(memory_space=pltpu.VMEM)
        dma = pltpu.SemaphoreType.DMA
        out, grad = pl.pallas_call(
            functools.partial(kernel, dims),
            out_shape=(
                pltpu.VMEM((32, 1024), BF16),
                pltpu.VMEM((4, 32), F32),
            ),
            in_specs=[hbm] * 7,
            out_specs=(vmem, vmem),
            scratch_shapes=[
                pltpu.VMEM((100, 1024), BF16),
                pltpu.VMEM((32, 100), BF16),
                pltpu.VMEM((8, 512, 512), BF16),
                pltpu.VMEM((8, 512, 512), BF16),
                pltpu.VMEM((2 * n_dom, 2, 16, 512), BF16),
                pltpu.VMEM((2 * n_dom, 2, 16, 512), BF16),
                pltpu.VMEM((n_col, 32, 1024), BF16),
                pltpu.VMEM((256, 1024), BF16),
                pltpu.VMEM((n_col, 32, 256), BF16),
                pltpu.VMEM((32, 256), BF16),
                pltpu.VMEM((n_col, 2, 16, 1024), BF16),
                pltpu.VMEM((n_x, 16, 128), F32),
                pltpu.VMEM((n_x, 16, 128), F32),
                pltpu.VMEM((n_z, 1, 128), F32),
                pltpu.VMEM((n_z, 1, 128), F32),
                dma((7,)),
                dma((2, n_dom, CHUNKS, n_dom)),
                dma((2, n_dom, CHUNKS)),
                dma((2, n_col)),
                dma((2, n_col)),
                dma((11,)),
                dma((11,)),
                dma((n_x,)),
                dma((n_x,)),
                dma((n_z,)),
                dma((n_z,)),
                pltpu.SemaphoreType.REGULAR,
                pltpu.SMEM((1, 3, 1, 8), jnp.int32),
                pltpu.SMEM((1, 1), jnp.int32),
            ],
            compiler_params=pltpu.CompilerParams(collective_id=0, has_side_effects=True),
        )(
            jnp.transpose(block_list, (0, 3, 1, 2)),
            block_count,
            features[0].T,
            w_in.T,
            w_hidden,
            blocks[0, 0],
            cotangent[0].T,
        )
        out, grad = pl.pallas_call(
            hand_over,
            out_shape=(
                jax.ShapeDtypeStruct((32, 1024), BF16),
                jax.ShapeDtypeStruct((4, 32), F32),
            ),
            in_specs=[vmem] * 2,
            out_specs=(hbm, hbm),
            scratch_shapes=[dma((2,))],
            compiler_params=pltpu.CompilerParams(vmem_limit_bytes=1024 * 1024),
        )(out, grad)
        return out.T[None], grad.T

    return jax.shard_map(
        body,
        mesh=mesh,
        in_specs=(
            P("rep", "dom", None),
            P(None, "col"),
            P("col", None),
            P("rep", "dom", None, None, None),
            P("rep", "dom", None, None),
            P("rep", "dom"),
            P("rep", "dom", "col"),
        ),
        out_specs=(P("rep", "dom", "col"), P("col", ("dom", "rep"))),
        check_vma=False,
    )
```

```python
import functools

import jax
import jax.numpy as jnp
from jax import lax
from jax.experimental import pallas as pl
from jax.experimental.pallas import tpu as pltpu
from jax.sharding import PartitionSpec as P

F32 = jnp.float32
BF16 = jnp.bfloat16
MESH = pl.DeviceIdType.MESH
NT = (((1,), (1,)), ((), ()))
CHUNKS = 1
PROGRAMS = {
    0: (('s', 0, 0, 1), ('s', 0, 0, 3), ('w', 3, 0, -1), ('s', 3, 0, 1), ('w', 1, 0, -1), ('s', 3, 0, 2), ('w', 2, 0, -1), ('w', 4, 0, -1), ('w', 5, 0, -1), ('w', 7, 0, -1), ('w', 6, 0, -1)),
    1: (('s', 1, 0, 4), ('s', 1, 0, 2), ('w', 0, 0, -1), ('s', 0, 0, 6), ('s', 1, 0, 0), ('w', 2, 0, -1), ('s', 2, 0, 0), ('w', 4, 0, -1), ('s', 4, 0, 3), ('s', 4, 0, 2), ('s', 4, 0, 0), ('s', 0, 0, 2), ('w', 7, 0, -1), ('s', 7, 0, 0), ('w', 3, 0, -1), ('w', 5, 0, -1), ('w', 6, 0, -1)),
    2: (('s', 2, 0, 5), ('s', 2, 0, 1), ('w', 1, 0, -1), ('s', 2, 0, 3), ('w', 5, 0, -1), ('s', 5, 0, 0), ('s', 5, 0, 3), ('s', 5, 0, 1), ('w', 4, 0, -1), ('w', 0, 0, -1), ('w', 6, 0, -1), ('w', 7, 0, -1), ('w', 3, 0, -1)),
    3: (('s', 3, 0, 6), ('s', 3, 0, 0), ('w', 0, 0, -1), ('s', 0, 0, 5), ('s', 0, 0, 4), ('w', 6, 0, -1), ('s', 6, 0, 0), ('s', 6, 0, 1), ('s', 6, 0, 4), ('s', 6, 0, 2), ('w', 2, 0, -1), ('w', 5, 0, -1), ('w', 1, 0, -1), ('w', 7, 0, -1), ('w', 4, 0, -1)),
    4: (('s', 4, 0, 1), ('s', 4, 0, 7), ('w', 1, 0, -1), ('s', 1, 0, 7), ('s', 1, 0, 6), ('s', 1, 0, 3), ('s', 1, 0, 5), ('w', 7, 0, -1), ('s', 7, 0, 2), ('s', 7, 0, 3), ('w', 5, 0, -1), ('w', 2, 0, -1), ('w', 0, 0, -1), ('w', 6, 0, -1), ('w', 3, 0, -1)),
    5: (('s', 5, 0, 2), ('s', 5, 0, 6), ('w', 6, 0, -1), ('s', 5, 0, 4), ('w', 2, 0, -1), ('s', 2, 0, 7), ('s', 2, 0, 4), ('s', 2, 0, 6), ('w', 3, 0, -1), ('w', 7, 0, -1), ('w', 1, 0, -1), ('w', 0, 0, -1), ('w', 4, 0, -1)),
    6: (('s', 6, 0, 3), ('s', 6, 0, 5), ('w', 7, 0, -1), ('s', 7, 0, 1), ('s', 6, 0, 7), ('w', 5, 0, -1), ('s', 5, 0, 7), ('w', 3, 0, -1), ('s', 3, 0, 4), ('s', 3, 0, 5), ('s', 3, 0, 7), ('s', 7, 0, 5), ('w', 0, 0, -1), ('s', 0, 0, 7), ('w', 4, 0, -1), ('w', 2, 0, -1), ('w', 1, 0, -1)),
    7: (('s', 7, 0, 6), ('s', 7, 0, 4), ('w', 4, 0, -1), ('s', 4, 0, 6), ('w', 6, 0, -1), ('s', 4, 0, 5), ('w', 5, 0, -1), ('w', 3, 0, -1), ('w', 2, 0, -1), ('w', 0, 0, -1), ('w', 1, 0, -1)),
}
PARTNERS = {0: (1, 2, 3), 1: (0, 2, 3, 4, 6), 2: (0, 1, 3, 4, 5), 3: (0, 1, 2, 4, 5, 6), 4: (1, 2, 3, 5, 6, 7), 5: (2, 3, 4, 6, 7), 6: (1, 3, 4, 5, 7), 7: (4, 5, 6)}


def gelu(v):
    return 0.5 * v * (1.0 + jnp.tanh(0.7978845608028654 * (v + 0.044715 * (v * v * v))))


def kernel(
    dims,
    list_hbm, count_hbm, feat_hbm, win_hbm, wh_hbm, blocks_hbm, ct_hbm,
    out_ref, grad_ref,
    feat, win, blocks, turned, z1, z2, ctb, ctp, wb, wct, gb, pb, rb, zb, zr,
    local_sem, line_send, line_recv, in_send, in_recv, ring_send, ring_recv,
    x_send, x_recv, z_send, z_recv, entered, lists, count,
):
    n_dom, n_col, n_x = dims
    n_y, n_z = n_col // 2, 2 * n_dom
    dom, col, rep = lax.axis_index("dom"), lax.axis_index("col"), lax.axis_index("rep")
    y, core = col // 2, col % 2
    z_hi, x = rep // n_x, rep % n_x
    z = z_hi * n_dom + dom

    def on_z(step):
        there = lax.rem(z + step, n_z)
        return {"dom": lax.rem(there, n_dom), "rep": (there // n_dom) * n_x + x}

    def on_x(step):
        return {"rep": z_hi * n_x + lax.rem(x + step, n_x)}

    def on_col(step):
        return {"col": lax.rem(col + step, n_col)}

    def on_y(step):
        return {"col": 2 * lax.rem(y + step, n_y) + core}

    sibling = {"col": 2 * y + 1 - core}

    def send(src, dst, send_sem, recv_sem, device):
        return pltpu.make_async_remote_copy(
            src_ref=src, dst_ref=dst, send_sem=send_sem, recv_sem=recv_sem,
            device_id=device, device_id_type=MESH,
        )

    loads = [
        pltpu.make_async_copy(feat_hbm, feat, local_sem.at[0]),
        pltpu.make_async_copy(win_hbm, win, local_sem.at[1]),
        pltpu.make_async_copy(ct_hbm, ctb.at[col], local_sem.at[2]),
        pltpu.make_async_copy(wh_hbm, wb.at[col], local_sem.at[3]),
        pltpu.make_async_copy(blocks_hbm, blocks, local_sem.at[4]),
        pltpu.make_async_copy(list_hbm, lists, local_sem.at[5]),
        pltpu.make_async_copy(count_hbm, count, local_sem.at[6]),
    ]
    for load in loads:
        load.start()

    barrier = pltpu.get_barrier_semaphore()
    for steps, place in ((n_x, on_x), (n_col, on_col)):
        def greet(step, carry, place=place):
            pl.semaphore_signal(barrier, inc=1, device_id=place(step), device_id_type=MESH)
            return carry

        lax.fori_loop(1, steps, greet, 0)
    for v in range(n_dom):
        @pl.when(dom == v)
        def _(v=v):
            for partner in PARTNERS[v]:
                pl.semaphore_signal(
                    barrier, inc=1, device_id={"dom": partner}, device_id_type=MESH
                )

    @pl.when(dom == 0)
    def _():
        pl.semaphore_signal(barrier, inc=1, device_id=on_z(n_z - 1), device_id_type=MESH)

    @pl.when(dom == n_dom - 1)
    def _():
        pl.semaphore_signal(barrier, inc=1, device_id=on_z(1), device_id_type=MESH)

    def piece(buf, src, chunk):
        if CHUNKS == 1:
            return buf.at[2 * src : 2 * src + 2]
        return buf.at[2 * src + chunk]

    def line_copy(e, buf, src, chunk, dst):
        part = piece(buf, src, chunk)
        return send(
            part, part, line_send.at[e, src, chunk, dst], line_recv.at[e, src, chunk], {"dom": dst}
        )

    def for_each_place(steps):
        for v in range(n_dom):
            @pl.when(dom == v)
            def _(v=v):
                steps(v, PROGRAMS[v])

    def line_start(e, buf):
        def steps(v, program):
            for kind, src, chunk, dst in program:
                if kind == "w":
                    return
                line_copy(e, buf, src, chunk, dst).start()

        for_each_place(steps)

    def line_pass(e, buf):
        def steps(v, program):
            waited = False
            for kind, src, chunk, dst in program:
                waited = waited or kind == "w"
                if kind == "w":
                    line_copy(e, buf, src, chunk, v).wait_recv()
                elif waited:
                    line_copy(e, buf, src, chunk, dst).start()

        for_each_place(steps)

    def line_drain(e, buf):
        def steps(v, program):
            for kind, src, chunk, dst in program:
                if kind == "s":
                    line_copy(e, buf, src, chunk, dst).wait_send()

        for_each_place(steps)

    def gather_copy(a, buf, step):
        return send(buf.at[col], buf.at[col], in_send.at[a, step], in_recv.at[a, col], on_col(step))

    def gather_arrival(a, buf, step):
        src = lax.rem(col + step, n_col)
        return send(buf.at[src], buf.at[src], in_send.at[a, step], in_recv.at[a, src], on_col(step))

    def spread(buf):
        total = jnp.zeros((64, 512), F32)
        for slot in range(8):
            used = slot < count[0, 0]
            row = lists[0, 0, 0, slot]
            part = buf[2 * lists[0, 1, 0, slot] + lists[0, 2, 0, slot]].reshape(32, 512)
            first = jnp.where(used & (row == 0), 1.0, 0.0)
            second = jnp.where(used & (row == 1), 1.0, 0.0)
            first = jnp.full((32, 512), first, F32).astype(BF16)
            second = jnp.full((32, 512), second, F32).astype(BF16)
            both = jnp.concatenate([part * first, part * second], axis=0)
            total = total + jnp.dot(both, turned[slot], preferred_element_type=F32)
        return total

    loads[0].wait()
    loads[1].wait()
    own = jnp.dot(win[...], feat[...], preferred_element_type=F32).astype(BF16)
    for j in range(2):
        for h in range(2):
            z1[2 * dom + j, h] = own[16 * h : 16 * h + 16, 512 * j : 512 * j + 512]

    for v in range(n_dom):
        @pl.when(dom == v)
        def _(v=v):
            ends = 1 if v in (0, n_dom - 1) else 0
            pl.semaphore_wait(barrier, len(PARTNERS[v]) + ends + (n_x - 1) + (n_col - 1))

    line_start(0, z1)

    loads[2].wait()
    loads[3].wait()
    for a, buf in ((0, wb), (1, ctb)):
        def start(step, carry, a=a, buf=buf):
            gather_copy(a, buf, step).start()
            return carry

        lax.fori_loop(1, n_col, start, 0)

    for load in loads[4:]:
        load.wait()

    def turn(slot, carry):
        turned[slot] = blocks[slot].T
        return carry

    lax.fori_loop(0, 8, turn, 0)
    line_pass(0, z1)

    @pl.when(dom == n_dom - 1)
    def _():
        pl.semaphore_signal(entered, inc=1, device_id=on_z(1), device_id_type=MESH)

    h1 = gelu(spread(z1)).astype(BF16)
    for j in range(2):
        for h in range(2):
            z2[2 * dom + j, h] = h1[32 * j + 16 * h : 32 * j + 16 * h + 16]

    @pl.when(dom == 0)
    def _():
        pl.semaphore_wait(entered, 1)

    line_start(1, z2)

    for a, buf in ((0, wb), (1, ctb)):
        def arrive(step, carry, a=a, buf=buf):
            gather_arrival(a, buf, step).wait_recv()
            return carry

        lax.fori_loop(1, n_col, arrive, 0)
    units = lax.broadcasted_iota(jnp.int32, (32, 256), 0) + 32 * col
    pick = (lax.broadcasted_iota(jnp.int32, (32, 256), 1) == units).astype(F32).astype(BF16)
    wct[...] = lax.dot_general(
        pick, wb[...].reshape(256, 256), NT, preferred_element_type=F32
    ).astype(BF16)
    place = lax.broadcasted_iota(jnp.int32, (256, 256), 0)
    wanted = 32 * (place & 7) + 16 * ((place >> 3) & 1) + 4 * ((place >> 4) & 3) + (place >> 6)
    order = (lax.broadcasted_iota(jnp.int32, (256, 256), 1) == wanted).astype(F32).astype(BF16)
    ctp[...] = jnp.dot(
        order, ctb[...].reshape(256, 1024), preferred_element_type=F32
    ).astype(BF16)

    line_pass(1, z2)
    g = spread(z2).astype(BF16)
    for j in range(2):
        for h in range(2):
            gb[col, h, :, 512 * j : 512 * j + 512] = g[32 * j + 16 * h : 32 * j + 16 * h + 16]

    def ring_copy(index, src, h, device):
        part = gb.at[src] if h is None else gb.at[src, h]
        return send(part, part, ring_send.at[index], ring_recv.at[index], device)

    before = 2 * lax.rem(y + n_y - 1, n_y) + core
    after = 2 * lax.rem(y + 1, n_y) + core
    across = 2 * lax.rem(y + 2, n_y) + core
    up, down = on_y(1), on_y(n_y - 1)
    other = 1 - 2 * core
    first = [
        ring_copy(0, col, 0, up), ring_copy(1, col, 1, down),
        ring_copy(2, col, 1, up), ring_copy(3, col, 0, down),
        ring_copy(4, col, None, sibling),
    ]

    for copy in first:
        copy.start()
    ga = jnp.concatenate([g[:32], g[32:]], axis=1)
    part = lax.dot_general(ctp[...], ga, NT, preferred_element_type=F32)
    packed = jnp.concatenate([part[64 * q : 64 * q + 64] for q in range(4)], axis=1)
    for t in range(n_x):
        pb[t] = packed[16 * t : 16 * t + 16]

    def x_copy(step):
        return send(
            pb.at[lax.rem(x + step, n_x)], rb.at[step], x_send.at[step], x_recv.at[step], on_x(step)
        )

    for step in range(1, n_x):
        x_copy(step).start()

    sums = pb[x]
    for step in range(1, n_x):
        x_copy(step).wait_recv()
        sums = sums + rb[step]
    for t in range(n_z):
        zb[t] = sums[t : t + 1]

    def z_copy(step):
        return send(
            zb.at[lax.rem(z + step, n_z)], zr.at[step], z_send.at[step], z_recv.at[step], on_z(step)
        )

    def z_start(step, carry):
        z_copy(step).start()
        return carry

    lax.fori_loop(1, n_z, z_start, 0)

    ring_copy(0, before, 0, up).wait_recv()
    second = [ring_copy(5, before, 0, up)]
    second[0].start()
    ring_copy(1, after, 1, down).wait_recv()
    second.append(ring_copy(6, after, 1, down))
    second[1].start()
    ring_copy(2, before, 1, up).wait_recv()
    second.append(ring_copy(7, before, None, sibling))
    second[2].start()
    ring_copy(3, after, 0, down).wait_recv()
    second.append(ring_copy(8, after, None, sibling))
    second[3].start()

    ring_copy(5, across, 0, up).wait_recv()
    third = [ring_copy(9, across, 0, sibling)]
    third[0].start()
    ring_copy(6, across, 1, down).wait_recv()
    third.append(ring_copy(10, across, 1, sibling))
    third[1].start()
    ring_copy(4, col + other, None, sibling).wait_recv()
    ring_copy(7, before + other, None, sibling).wait_recv()
    ring_copy(8, after + other, None, sibling).wait_recv()
    ring_copy(9, across + other, 0, sibling).wait_recv()
    ring_copy(10, across + other, 1, sibling).wait_recv()
    out_ref[...] = jnp.dot(
        wct[...], gb[...].reshape(256, 1024), preferred_element_type=F32
    ).astype(BF16)

    for copy in first + second + third:
        copy.wait_send()
    for step in range(1, n_x):
        x_copy(step).wait_send()

    for a, buf in ((0, wb), (1, ctb)):
        def done(step, carry, a=a, buf=buf):
            gather_copy(a, buf, step).wait_send()
            return carry

        lax.fori_loop(1, n_col, done, 0)
    line_drain(0, z1)
    line_drain(1, z2)

    def z_add(step, total):
        z_copy(step).wait_recv()
        return total + zr[step]

    total = lax.fori_loop(1, n_z, z_add, zb[z])
    for q in range(4):
        grad_ref[q : q + 1, :] = total[:, 32 * q : 32 * q + 32]

    def z_done(step, carry):
        z_copy(step).wait_send()
        return carry

    lax.fori_loop(1, n_z, z_done, 0)


def hand_over(out_held, grad_held, out_ref, grad_ref, sems):
    copies = [
        pltpu.make_async_copy(out_held, out_ref, sems.at[0]),
        pltpu.make_async_copy(grad_held, grad_ref, sems.at[1]),
    ]
    for copy in copies:
        copy.start()
    for copy in copies:
        copy.wait()


def solution(mesh):
    n_dom, n_col = mesh.shape["dom"], mesh.shape["col"]
    n_x = mesh.shape["rep"] // 2
    dims = (n_dom, n_col, n_x)
    n_z = 2 * n_dom

    def body(features, w_in, w_hidden, blocks, block_list, block_count, cotangent):
        hbm = pl.BlockSpec(memory_space=pltpu.HBM)
        vmem = pl.BlockSpec(memory_space=pltpu.VMEM)
        dma = pltpu.SemaphoreType.DMA
        out, grad = pl.pallas_call(
            functools.partial(kernel, dims),
            out_shape=(
                pltpu.VMEM((32, 1024), BF16),
                pltpu.VMEM((4, 32), F32),
            ),
            in_specs=[hbm] * 7,
            out_specs=(vmem, vmem),
            scratch_shapes=[
                pltpu.VMEM((100, 1024), BF16),
                pltpu.VMEM((32, 100), BF16),
                pltpu.VMEM((8, 512, 512), BF16),
                pltpu.VMEM((8, 512, 512), BF16),
                pltpu.VMEM((2 * n_dom, 2, 16, 512), BF16),
                pltpu.VMEM((2 * n_dom, 2, 16, 512), BF16),
                pltpu.VMEM((n_col, 32, 1024), BF16),
                pltpu.VMEM((256, 1024), BF16),
                pltpu.VMEM((n_col, 32, 256), BF16),
                pltpu.VMEM((32, 256), BF16),
                pltpu.VMEM((n_col, 2, 16, 1024), BF16),
                pltpu.VMEM((n_x, 16, 128), F32),
                pltpu.VMEM((n_x, 16, 128), F32),
                pltpu.VMEM((n_z, 1, 128), F32),
                pltpu.VMEM((n_z, 1, 128), F32),
                dma((7,)),
                dma((2, n_dom, CHUNKS, n_dom)),
                dma((2, n_dom, CHUNKS)),
                dma((2, n_col)),
                dma((2, n_col)),
                dma((11,)),
                dma((11,)),
                dma((n_x,)),
                dma((n_x,)),
                dma((n_z,)),
                dma((n_z,)),
                pltpu.SemaphoreType.REGULAR,
                pltpu.SMEM((1, 3, 1, 8), jnp.int32),
                pltpu.SMEM((1, 1), jnp.int32),
            ],
            compiler_params=pltpu.CompilerParams(collective_id=0, has_side_effects=True),
        )(
            jnp.transpose(block_list, (0, 3, 1, 2)),
            block_count,
            features[0].T,
            w_in.T,
            w_hidden,
            blocks[0, 0],
            cotangent[0].T,
        )
        out, grad = pl.pallas_call(
            hand_over,
            out_shape=(
                jax.ShapeDtypeStruct((32, 1024), BF16),
                jax.ShapeDtypeStruct((4, 32), F32),
            ),
            in_specs=[vmem] * 2,
            out_specs=(hbm, hbm),
            scratch_shapes=[dma((2,))],
            compiler_params=pltpu.CompilerParams(vmem_limit_bytes=1024 * 1024),
        )(out, grad)
        return out.T[None], grad.T

    return jax.shard_map(
        body,
        mesh=mesh,
        in_specs=(
            P("rep", "dom", None),
            P(None, "col"),
            P("col", None),
            P("rep", "dom", None, None, None),
            P("rep", "dom", None, None),
            P("rep", "dom"),
            P("rep", "dom", "col"),
        ),
        out_specs=(P("rep", "dom", "col"), P("col", ("dom", "rep"))),
        check_vma=False,
    )
```
